32 devices in a mesh: basin: 2 (over x), recv: 8 (over z, y), src: 2 (over core).
Axes of the slice: x: 2, y: 2, z: 4, core: 2. Of those that a mesh axis runs over, the one named last changes fastest.
Arguments:
- positions: float32 [3, 4096], P(None, ('basin', 'recv', 'src')), parts along dimension 1, may hold values from -1.1 to 1.1, as said below
- normals: float32 [3, 4096], P(None, ('basin', 'recv', 'src')), parts along dimension 1, may hold values from -1 to 1, as said below
- area: float32 [4096], P(('basin', 'recv', 'src')), parts along dimension 0, may hold values from 0.0009765625 to 0.0078125
- albedo: float32 [4096], P(('basin', 'recv', 'src')), parts along dimension 0, may hold values from 0.1 to 0.6
- conductivity: float32 [4096], P(('basin', 'recv', 'src')), parts along dimension 0, may hold values from 0.05 to 0.4
- soil: float32 [32, 4096], P(None, ('basin', 'recv', 'src')), parts along dimension 1, may hold values from 0.5 to 1.2
- sun_tan: float32 [16], replicated, may hold values from 0.05 to 2
- samples: int32 [32, 32], P(('basin', 'recv', 'src')), parts along dimension 0, may hold values from 1 to 2047
- occupancy: int32 [32, 16], P('basin'), parts along dimension 0, may hold values 0 or 1
Outputs:
- soil_final: float32 [32, 4096], P(None, ('basin', 'recv', 'src')), parts along dimension 1
- bounce: float32 [16, 4096], P(None, ('basin', 'recv', 'src')), parts along dimension 1
The draws below stay inside these ranges and needn't reach their ends.
There are 2 independent parts, one for each index of `basin`. The reference program is written for one: setup_inputs(seed, part) draws one part's arguments, and reference() takes and returns one part's arrays. A program takes and returns all parts, laid end to end along the dimension named above; an argument that names none is the same for every part. Nothing has to cross between parts.
Inputs may be any that keep to these rules, and one draw needn't show every extreme that they name: `positions`: facets lie on a bowl below z = 0. `normals`: each column has unit length.
All inputs are finite; a program needn't handle non-finite values.
Results may differ from the reference program's by a relative error of at most 0.0003.
Values may be sent and summed in bfloat16 or wider, within the bound.
A program may use at most 64 MiB of HBM per device.

```python
import math
import jax
import jax.numpy as jnp
from jax import lax

FAC = 128
SAMPLES = 32
LAYERS = 32
F = 2048
AZIMUTHS = 16
EPOCHS = 16
BLOCKS = 16


def bowl_shape(key):
    base = jax.random.fold_in(key, 31)
    first, second, third, fourth_key = jax.random.split(base, 4)
    turn = jax.random.uniform(first, (F,), jnp.float32, 0.0, 2.0 * math.pi)
    depth = jax.random.uniform(second, (F,), jnp.float32, 0.0, 1.0)
    radius = jax.random.uniform(third, (F,), jnp.float32, 0.9, 1.1)
    side = jnp.sqrt(1.0 - depth * depth)
    unit = jnp.stack([side * jnp.cos(turn), side * jnp.sin(turn), -depth])
    jitter = jax.random.uniform(fourth_key, (3, F), jnp.float32, -0.3, 0.3)
    facing = jitter - unit
    facing = facing / jnp.sqrt(jnp.sum(facing * facing, axis=0, keepdims=True))
    return (radius[None, :] * unit, facing)


def draw_positions(key, part):
    return bowl_shape(key)[0]


def draw_normals(key, part):
    return bowl_shape(key)[1]


def touch_ends(result, own_key, smallest, top_value):
    extent = result.shape
    index_at = [jax.random.randint(jax.random.fold_in(own_key, axis), (), 0, extent[axis]) for axis in range(len(extent))]
    result = result.at[tuple(index_at)].set(smallest)
    longest = extent.index(max(extent))
    index_at[longest] = (index_at[longest] + 1) % extent[longest]
    return result.at[tuple(index_at)].set(top_value)


def shard_levels(own_key, shape, cuts, smallest, top_value):
    loudness = 1.0
    for dim, blocks in cuts:
        steps = jax.random.uniform(jax.random.fold_in(jax.random.fold_in(own_key, 6), dim), (blocks,), jnp.float32, smallest / len(cuts), top_value / len(cuts))
        loudness = loudness * jnp.repeat(jnp.exp(steps), shape[dim] // blocks).reshape((-1,) + (1,) * (len(shape) - 1 - dim))
    return loudness


def setup_inputs(seed: int = 0, part: int = 0) -> dict:
    arg_keys = jax.random.split(jax.random.key(seed), 10)
    own_keys = jax.random.split(jax.random.fold_in(arg_keys[9], part), 10)
    return {
        "positions": draw_positions(jax.random.fold_in(jax.random.fold_in(arg_keys[9], part), 71), part),
        "normals": draw_normals(jax.random.fold_in(jax.random.fold_in(arg_keys[9], part), 71), part),
        "area": jnp.clip(jnp.exp(math.log(0.0078125) - 2.0794415 * jax.random.uniform(own_keys[2], (F,), jnp.float32) ** shard_levels(own_keys[2], (F,), ((0, 16),), -0.2, 0.2)), 0.0009765625, 0.0078125),
        "albedo": jnp.clip(0.1 + 0.5 * jax.random.uniform(own_keys[3], (F,), jnp.float32) ** shard_levels(own_keys[3], (F,), ((0, 16),), -0.2, 0.2), 0.1, 0.6),
        "conductivity": jnp.clip(jnp.exp(math.log(0.4) - 2.0794415 * jax.random.uniform(own_keys[4], (F,), jnp.float32) ** shard_levels(own_keys[4], (F,), ((0, 16),), -0.2, 0.2)), 0.05, 0.4),
        "soil": jnp.clip(0.5 + 0.70000005 * jax.random.uniform(own_keys[5], (LAYERS, F), jnp.float32) ** shard_levels(own_keys[5], (LAYERS, F), ((1, 16),), -0.2, 0.2), 0.5, 1.2),
        "sun_tan": jnp.clip(jax.random.uniform(arg_keys[6], (EPOCHS,), jnp.float32, 0.05, 2.0), 0.05, 2.0),
        "samples": touch_ends(jax.random.randint(own_keys[7], (AZIMUTHS, SAMPLES), 1, min(F, 4096)), jax.random.fold_in(own_keys[7], 1), 1, (min(F, 4096)) - 1).astype(jnp.int32),
        "occupancy": touch_ends((jax.random.randint(own_keys[8], (BLOCKS, BLOCKS), 0, 3) < 2).astype(jnp.int32), jax.random.fold_in(own_keys[8], 1), 0, 1),
    }


solar_flux = 2.0
emissivity = 0.9
surface_gain = 0.1
shade_width = 0.1
reach_offset = 0.05

def fourth(value):
    square = value * value
    return square * square

def rotate(values, shift):
    count = values.shape[0]
    doubled = jnp.concatenate([values, values], 0)
    return lax.dynamic_slice_in_dim(doubled, shift.astype(jnp.int32), count, 0)

def profile_max(coords, offsets):
    px, py, pz = (coords[0], coords[1], coords[2])
    count = px.shape[0]

    def sweep(best, shift):
        delta_x = rotate(px, shift) - px
        delta_y = rotate(py, shift) - py
        reach = jnp.sqrt(delta_x * delta_x + delta_y * delta_y) + reach_offset
        slope = (rotate(pz, shift) - pz) / reach
        return (jnp.maximum(best, slope), None)
    start = jnp.full((count,), -1e+30, jnp.float32)
    best, unused = lax.scan(sweep, start, offsets.astype(jnp.int32))
    return best

def sunlight(facing, sun_tan, horizon):
    count = sun_tan.shape[0]
    angle = 2.0 * math.pi * jnp.arange(count, dtype=jnp.float32) / count
    elevation = jnp.arctan(sun_tan)
    sun_x = jnp.cos(elevation) * jnp.cos(angle)
    sun_y = jnp.cos(elevation) * jnp.sin(angle)
    sun_z = jnp.sin(elevation)
    incidence = sun_x[:, None] * facing[0][None, :] + sun_y[:, None] * facing[1][None, :] + sun_z[:, None] * facing[2][None, :]
    shade = jax.nn.sigmoid((sun_tan[:, None] - horizon) / shade_width)
    return solar_flux * jnp.maximum(incidence, 0.0) * shade

def conduct(soil, direct, bounce, albedo, conductivity):

    def advance(temps, inputs):
        light, scattered = inputs
        grad = temps[1:] - temps[:-1]
        edge = jnp.zeros((1, temps.shape[1]), jnp.float32)
        change = jnp.concatenate([grad, edge], 0) - jnp.concatenate([edge, grad], 0)
        temps = temps + conductivity[None, :] * change
        absorbed = (1.0 - albedo) * (light + scattered)
        top = temps[0] + surface_gain * (absorbed - emissivity * fourth(temps[0]))
        return (jnp.concatenate([top[None, :], temps[1:]], 0), None)
    final, unused = lax.scan(advance, soil, (direct, bounce))
    return final

def reference(positions, normals, area, albedo, conductivity, soil, sun_tan, samples, occupancy):
    horizon = lax.map(lambda offsets: profile_max(positions, offsets), samples)
    direct = sunlight(normals, sun_tan, horizon)
    radiance = (albedo[None, :] * direct + emissivity * fourth(soil[0])[None, :]).astype(jnp.bfloat16)
    table = occupancy.astype(jnp.float32)

    def per_block(block):
        start = (block * FAC).astype(jnp.int32)
        rec_pos = lax.dynamic_slice_in_dim(positions, start, FAC, 1)
        rec_nrm = lax.dynamic_slice_in_dim(normals, start, FAC, 1)
        weight = jnp.repeat(lax.dynamic_index_in_dim(table, block, 0, keepdims=False), FAC)[:, None]
        delta_x = positions[0][:, None] - rec_pos[0][None, :]
        delta_y = positions[1][:, None] - rec_pos[1][None, :]
        delta_z = positions[2][:, None] - rec_pos[2][None, :]
        facing = jnp.maximum(rec_nrm[0][None, :] * delta_x + rec_nrm[1][None, :] * delta_y + rec_nrm[2][None, :] * delta_z, 0.0)
        toward = jnp.maximum(-(normals[0][:, None] * delta_x + normals[1][:, None] * delta_y + normals[2][:, None] * delta_z), 0.0)
        spread = delta_x * delta_x + delta_y * delta_y + delta_z * delta_z + area[:, None]
        view = (facing * toward * area[:, None] * weight / (math.pi * spread * spread)).astype(jnp.bfloat16)
        return jnp.dot(radiance, view, preferred_element_type=jnp.float32)
    pieces = lax.map(per_block, jnp.arange(BLOCKS, dtype=jnp.int32))
    bounce = jnp.transpose(pieces, (1, 0, 2)).reshape(EPOCHS, F)
    final = conduct(soil, direct, bounce, albedo, conductivity)
    return (final, bounce)
```

```python
import functools
import math

import jax
import jax.numpy as jnp
from jax import lax
from jax.experimental import pallas as pl
from jax.experimental.pallas import tpu as pltpu
from jax.sharding import PartitionSpec as P

solar_flux = 2.0
emissivity = 0.9
surface_gain = 0.1
shade_width = 0.1
reach_offset = 0.05
GROUP = 8
CHUNK = 16
TURNS = 32


def fourth(value):
    square = value * value
    return square * square


def column(row, count):
    wide = jnp.broadcast_to(row[:, :count], (count, count))
    here = lax.broadcasted_iota(jnp.int32, (count, count), 0) == lax.broadcasted_iota(
        jnp.int32, (count, count), 1
    )
    return jnp.sum(jnp.where(here, wide, 0.0), axis=1, keepdims=True)


def kernel(
    n_recv,
    n_src,
    pos_in,
    nrm_in,
    area_in,
    alb_in,
    cond_in,
    soil_in,
    tan_in,
    smp_in,
    occ_in,
    bounce_ref,
    heat_ref,
    cond_ref,
    soil_ref,
    pos_ref,
    nrm_ref,
    area_ref,
    alb_ref,
    tan_ref,
    smp_ref,
    occ_ref,
    near,
    far,
    planes,
    shifts,
    cols,
    view,
    direct_ref,
    lit_ref,
    tall_tan,
    radg,
    sems,
    loads,
):
    n = n_recv * n_src
    width = pos_ref.shape[1]
    n_samples = smp_ref.shape[1]
    epochs = tan_ref.shape[1]
    bits = width.bit_length() - 1
    few = n <= 16
    me = lax.axis_index("recv") * n_src + lax.axis_index("src")

    def peer(k):
        p = (me + (n - k)) & (n - 1)
        return {"recv": p >> (n_src.bit_length() - 1), "src": p & (n_src - 1)}

    def over(first, last, step):
        if few:
            for k in sorted(range(first, last), key=lambda k: abs(2 * k - n)):
                step(k)
        else:
            lax.fori_loop(first, last, lambda k, c: (step(k), c)[1], 0)

    barrier = pltpu.get_barrier_semaphore()
    over(
        1,
        n,
        lambda k: pl.semaphore_signal(
            barrier, inc=1, device_id=peer(k), device_id_type=pl.DeviceIdType.MESH
        ),
    )
    pairs = (
        (pos_in, pos_ref),
        (smp_in, smp_ref),
        (nrm_in, nrm_ref),
        (area_in, area_ref),
        (tan_in, tan_ref),
        (soil_in, soil_ref),
        (alb_in, alb_ref),
        (cond_in, cond_ref),
        (occ_in.at[pl.ds(me, 1)], occ_ref),
    )
    fetched = [
        pltpu.make_async_copy(there, here, loads.at[i]) for i, (there, here) in enumerate(pairs)
    ]
    for copy in fetched:
        copy.start()
    for copy in fetched[:4]:
        copy.wait()
    near[0, 0:3, :] = pos_ref[...]
    near[0, 3:4, 0:n_samples] = smp_ref[...].astype(jnp.float32)
    far[0, 0:3, :] = nrm_ref[...]
    far[0, 3:4, :] = area_ref[...]
    for copy in fetched[4:]:
        copy.wait()
    pl.semaphore_wait(barrier, n - 1)

    def send(ref, k, which):
        pltpu.make_async_remote_copy(
            src_ref=ref.at[0],
            dst_ref=ref.at[k],
            send_sem=sems.at[which],
            recv_sem=sems.at[which + 1],
            device_id=peer(k),
            device_id_type=pl.DeviceIdType.MESH,
        ).start()

    def everyone(ref, which):
        return pltpu.make_async_remote_copy(
            src_ref=ref.at[pl.ds(1, n - 1)],
            dst_ref=ref.at[pl.ds(1, n - 1)],
            send_sem=sems.at[which],
            recv_sem=sems.at[which + 1],
            device_id=peer(1),
            device_id_type=pl.DeviceIdType.MESH,
        )

    over(1, n, lambda k: send(near, k, 0))
    over(1, n, lambda k: send(far, k, 4))

    mine = near[0]
    tall = jnp.transpose(jnp.concatenate([mine, far[0]], axis=0))
    for c, at in enumerate((0, 1, 2, 4, 5, 6)):
        cols[c] = jnp.broadcast_to(tall[:, at : at + 1], (width, width))
    tan = column(tan_ref[...], epochs)
    angle = (
        2.0
        * math.pi
        * lax.broadcasted_iota(jnp.int32, (epochs, width), 0).astype(jnp.float32)
        / epochs
    )
    cos_e = 1.0 / jnp.sqrt(1.0 + tan * tan)
    incidence = (
        cos_e * jnp.cos(angle) * nrm_ref[0:1, :]
        + cos_e * jnp.sin(angle) * nrm_ref[1:2, :]
        + tan * cos_e * nrm_ref[2:3, :]
    )
    lit_ref[...] = solar_flux * jnp.maximum(incidence, 0.0)
    tall_tan[...] = jnp.broadcast_to(tan, (epochs, width))
    infrared = emissivity * fourth(soil_ref[0:1, :])

    everyone(near, 0).wait_recv()
    for c in range(3):
        planes[c] = near[:, c, :]
    rows = near[:, 3, :]
    shifts[0:n, :] = rows
    shifts[n : 2 * n, :] = rows

    lane = lax.broadcasted_iota(jnp.int32, (GROUP, width), 1)
    px, py, pz = (jnp.broadcast_to(mine[c : c + 1, :], (GROUP, width)) for c in range(3))

    def azimuths(group):
        offset = n - me + group * GROUP
        steps = shifts[pl.ds(offset, GROUP), :].astype(jnp.int32)
        best = jnp.full((GROUP, width), -1e30, jnp.float32)
        for s in range(n_samples):
            shift = jnp.broadcast_to(steps[:, s : s + 1], (GROUP, width))
            row = ((shift + (width - 1) - lane) >> bits) & (n - 1)
            within = row & (GROUP - 1)
            part = row >> (GROUP.bit_length() - 1)
            turn = (lane + shift) & (width - 1)
            found = []
            for c in range(3):
                picked = None
                for g in range(n // GROUP):
                    block = planes[c, g * GROUP : (g + 1) * GROUP, :]
                    got = jnp.take_along_axis(block, within, axis=0)
                    picked = got if picked is None else jnp.where(part == g, got, picked)
                found.append(jnp.take_along_axis(picked, turn, axis=1))
            dx = found[0] - px
            dy = found[1] - py
            reach = jnp.sqrt(dx * dx + dy * dy) + reach_offset
            best = jnp.maximum(best, (found[2] - pz) / reach)
        start = group * GROUP
        here = pl.ds(start if few else pl.multiple_of(start, GROUP), GROUP)
        direct = lit_ref[here, :] * jax.nn.sigmoid((tall_tan[here, :] - best) / shade_width)
        direct_ref[here, :] = direct
        radg[0, group] = (alb_ref[...] * direct + infrared).astype(jnp.bfloat16)
        over(1, n, lambda k: send(radg.at[:, group], k, 2))

    over(0, n // GROUP, azimuths)

    def see(k, carry):
        weight = occ_ref[0, lax.rem(me + k, n)].astype(jnp.float32)
        sx, sy, sz = (near[k, c : c + 1, :] for c in range(3))
        ox, oy, oz, size = (far[k, c : c + 1, :] for c in range(4))
        scale = size * weight / math.pi
        for i in range(width // CHUNK):
            at = slice(i * CHUNK, (i + 1) * CHUNK)
            dx = sx - cols[0, at, :]
            dy = sy - cols[1, at, :]
            dz = sz - cols[2, at, :]
            facing = cols[3, at, :] * dx + cols[4, at, :] * dy + cols[5, at, :] * dz
            toward = -(ox * dx + oy * dy + oz * dz)
            spread = dx * dx + dy * dy + dz * dz + size
            seen = jnp.maximum(facing, 0.0) * jnp.maximum(toward, 0.0) * scale
            view[k, at, :] = (seen / (spread * spread)).astype(jnp.bfloat16)
        return carry

    everyone(far, 4).wait_recv()
    lax.fori_loop(0, n, see, 0)
    everyone(radg, 2).wait_recv()

    def fold(k, total):
        sent = jnp.concatenate([radg[k, g] for g in range(epochs // GROUP)], axis=0)
        return total + lax.dot_general(
            sent, view[k], (((1,), (1,)), ((), ())), preferred_element_type=jnp.float32
        )

    total = jnp.zeros((epochs, width), jnp.float32)
    if few:
        for k in range(n):
            total = fold(k, total)
    else:
        total = lax.fori_loop(0, n, fold, total)
    bounce_ref[...] = total
    keep = surface_gain * (1.0 - alb_ref[...])
    heat_ref[...] = keep * (direct_ref[...] + total)
    everyone(near, 0).wait_send()
    everyone(far, 4).wait_send()
    everyone(radg, 2).wait_send()


def step(
    n_recv,
    n_src,
    pos_in,
    nrm_in,
    area_in,
    alb_in,
    cond_in,
    soil_in,
    tan_in,
    smp_in,
    occ_in,
    bounce_ref,
    heat_ref,
    cond_ref,
    soil_ref,
    alb_ref,
    tan_ref,
    occ_ref,
    near,
    far,
    smp,
    planes,
    table,
    cols,
    view,
    sun_ref,
    direct_ref,
    lit_ref,
    hello,
    sent,
    got,
    loads,
):
    n = n_recv * n_src
    width = alb_ref.shape[1]
    n_samples = smp.shape[2]
    epochs = tan_ref.shape[1]
    bits = width.bit_length() - 1
    rows = 2 * n
    me = lax.axis_index("recv") * n_src + lax.axis_index("src")

    def device(p):
        return {"recv": p >> (n_src.bit_length() - 1), "src": p & (n_src - 1)}

    def greet(sem, p):
        pl.semaphore_signal(sem, inc=1, device_id=device(p), device_id_type=pl.DeviceIdType.MESH)

    def each(first, last, do):
        lax.fori_loop(first, last, lambda p, c: (do(p), c)[1], 0)

    own = pl.ds(me, 1)
    pairs = [(pos_in.at[pl.ds(c, 1)], near.at[c, own]) for c in range(3)]
    pairs += [(smp_in, smp.at[me])]
    pairs += [(nrm_in.at[pl.ds(c, 1)], far.at[c, own]) for c in range(3)]
    pairs += [(area_in, far.at[3, own]), (alb_in, far.at[4, own]), (soil_in.at[pl.ds(0, 1)], far.at[5, own])]
    pairs += [
        (alb_in, alb_ref),
        (tan_in, tan_ref),
        (soil_in, soil_ref),
        (cond_in, cond_ref),
        (occ_in.at[own], occ_ref),
    ]
    fetched = [
        pltpu.make_async_copy(there, here, loads.at[i]) for i, (there, here) in enumerate(pairs)
    ]
    for copy in fetched:
        copy.start()
    barrier = pltpu.get_barrier_semaphore()
    each(me + 1, n, lambda p: greet(barrier, p))
    pl.when(me > 0)(lambda: pl.semaphore_wait(barrier, me))
    each(0, me, lambda p: greet(hello.at[me], p))

    def parts(p, which):
        ref = (near, smp, far)[which]
        return ref.at[p] if which == 1 else ref.at[:, pl.ds(p, 1)]

    def remote(slot, to, which):
        return pltpu.make_async_remote_copy(
            src_ref=parts(slot, which),
            dst_ref=parts(slot, which),
            send_sem=sent.at[which],
            recv_sem=got.at[which, slot],
            device_id=device(to),
            device_id_type=pl.DeviceIdType.MESH,
        )

    for copy in fetched[:4]:
        copy.wait()

    def first(p):
        remote(me, p, 0).start()
        remote(me, p, 1).start()

    each(0, me, first)
    for copy in fetched[4:10]:
        copy.wait()
    each(0, me, lambda p: remote(me, p, 2).start())
    for copy in fetched[10:]:
        copy.wait()

    mine = jnp.concatenate([near[:, me, :], far[0:3, me, :]], axis=0)
    mine = jnp.concatenate([mine, mine[0:2]], axis=0)
    tall = jnp.transpose(mine)
    for c in range(6):
        cols[c] = jnp.broadcast_to(tall[:, c : c + 1], (width, width))
    tan = column(tan_ref[...], epochs)
    angle = (
        2.0
        * math.pi
        * lax.broadcasted_iota(jnp.int32, (epochs, width), 0).astype(jnp.float32)
        / epochs
    )
    cos_e = 1.0 / jnp.sqrt(1.0 + tan * tan)
    sun_ref[0] = cos_e * jnp.cos(angle)
    sun_ref[1] = cos_e * jnp.sin(angle)
    sun_ref[2] = jnp.broadcast_to(tan * cos_e, (epochs, width))
    sun_ref[3] = jnp.broadcast_to(tan, (epochs, width))

    def answer(p):
        pl.semaphore_wait(hello.at[p], 1)
        remote(me, p, 0).start()
        remote(me, p, 1).start()
        remote(me, p, 2).start()

    each(me + 1, n, answer)

    def see(p):
        weight = occ_ref[0, p].astype(jnp.float32)
        row = pl.ds(p, 1)
        sx, sy, sz = (near[c, row, :] for c in range(3))
        ox, oy, oz, size = (far[c, row, :] for c in range(4))
        scale = size * weight / math.pi
        for i in range(width // CHUNK):
            at = slice(i * CHUNK, (i + 1) * CHUNK)
            dx = sx - cols[0, at, :]
            dy = sy - cols[1, at, :]
            dz = sz - cols[2, at, :]
            facing = cols[3, at, :] * dx + cols[4, at, :] * dy + cols[5, at, :] * dz
            toward = -(ox * dx + oy * dy + oz * dz)
            spread = dx * dx + dy * dy + dz * dz + size
            seen = jnp.maximum(facing, 0.0) * jnp.maximum(toward, 0.0) * scale
            view[p, at, :] = (seen / (spread * spread)).astype(jnp.bfloat16)

    early = n - n // 8

    def arrive(m):
        p = me ^ m
        for which in range(3):
            remote(p, p, which).wait_recv()
        see(p)

    see(me)
    each(1, early, arrive)
    each(early, n, lambda m: [remote(me ^ m, me ^ m, which).wait_recv() for which in range(2)] and None)

    for c in range(3):
        planes[c, 0:n, :] = near[c]
        planes[c, n : n + 8, :] = near[c, 0:8]
    lane = lax.broadcasted_iota(jnp.int32, (8, width), 1)

    def spin(i, carry):
        for j in range(TURNS):
            r = i * TURNS + j
            whole = lane >= r
            back = (width - r) & (width - 1)
            for c in range(3):
                for g in range(n // 8):
                    here = planes[c, g * 8 : g * 8 + 8, :]
                    after = planes[c, g * 8 + 1 : g * 8 + 9, :]
                    turned = pltpu.roll(jnp.where(whole, here, after), back, 1)
                    table[c, pl.ds(r * rows + g * 8, 8), :] = turned
                    table[c, pl.ds(r * rows + n + g * 8, 8), :] = turned
        return carry

    lax.fori_loop(0, width // TURNS, spin, 0)

    def horizons(a, carry):
        here = [[planes[c, g * 8 : g * 8 + 8, :] for g in range(n // 8)] for c in range(3)]
        best = [jnp.full((8, width), -1e30, jnp.float32) for g in range(n // 8)]
        for s in range(n_samples):
            shift = smp[a, 0, s]
            start = (shift & (width - 1)) * rows + (shift >> bits)
            for g in range(n // 8):
                fx, fy, fz = (table[c, pl.ds(start + g * 8, 8), :] for c in range(3))
                dx = fx - here[0][g]
                dy = fy - here[1][g]
                square = jnp.maximum(dx * dx + dy * dy, 1e-30)
                reach = square * lax.rsqrt(square) + reach_offset
                best[g] = jnp.maximum(best[g], (fz - here[2][g]) / reach)
        line = pl.ds(a, 1)
        cx, cy, cz, tans = (sun_ref[c, line, :] for c in range(4))
        for g in range(n // 8):
            at = slice(g * 8, g * 8 + 8)
            incidence = cx * far[0, at, :] + cy * far[1, at, :] + cz * far[2, at, :]
            shade = jax.nn.sigmoid((tans - best[g]) / shade_width)
            direct = solar_flux * jnp.maximum(incidence, 0.0) * shade
            direct_ref[a, at, :] = direct
            lit_ref[a, at, :] = far[4, at, :] * direct + emissivity * fourth(far[5, at, :])
        return carry

    def last(m):
        remote(me ^ m, me ^ m, 2).wait_recv()
        see(me ^ m)

    each(early, n, last)
    lax.fori_loop(0, epochs, horizons, 0)

    total = jnp.zeros((epochs, width), jnp.float32)
    for p in range(n):
        total = total + lax.dot_general(
            lit_ref[:, p, :].astype(jnp.bfloat16),
            view[p],
            (((1,), (1,)), ((), ())),
            preferred_element_type=jnp.float32,
        )
    bounce_ref[...] = total
    keep = surface_gain * (1.0 - alb_ref[...])
    heat_ref[...] = keep * (direct_ref[:, me, :] + total)
    each(1, n, lambda m: [remote(me, me, which).wait_send() for which in range(3)] and None)


def conduct(bounce_in, heat_ref, cond_ref, soil_ref, final_ref, bounce_ref):
    layers, width = soil_ref.shape
    epochs = heat_ref.shape[0]
    bounce_ref[...] = bounce_in[...]
    cond = cond_ref[...]
    first = lax.broadcasted_iota(jnp.int32, (layers, width), 0) == 0
    last = lax.broadcasted_iota(jnp.int32, (layers, width), 0) == layers - 1

    def advance(t, temps):
        below = jnp.where(last, temps, pltpu.roll(temps, layers - 1, 0))
        above = jnp.where(first, temps, pltpu.roll(temps, 1, 0))
        temps = temps + cond * ((below - temps) - (temps - above))
        gain = heat_ref[pl.ds(t, 1), :] - (surface_gain * emissivity) * fourth(temps)
        return jnp.where(first, temps + gain, temps)

    temps = soil_ref[...]
    if epochs <= 16:
        for t in range(epochs):
            temps = advance(t, temps)
    else:
        temps = lax.fori_loop(0, epochs, advance, temps)
    final_ref[...] = temps


def body(positions, normals, area, albedo, conductivity, soil, sun_tan, samples, occupancy):
    n_recv = lax.axis_size("recv")
    n_src = lax.axis_size("src")
    n = n_recv * n_src
    width = positions.shape[1]
    epochs = sun_tan.shape[0]
    vmem = pl.BlockSpec(memory_space=pltpu.VMEM)
    f32 = jnp.float32
    n_samples = samples.shape[1]
    if n <= 16:
        program = step
        scratch = [
            pltpu.VMEM((1, width), f32),
            pltpu.VMEM((1, epochs), f32),
            pltpu.SMEM((1, occupancy.shape[1]), jnp.int32),
            pltpu.VMEM((3, n, width), f32),
            pltpu.VMEM((6, n, width), f32),
            pltpu.SMEM((n, 1, n_samples), jnp.int32),
            pltpu.VMEM((3, n + 8, width), f32),
            pltpu.VMEM((3, width * 2 * n, width), f32),
            pltpu.VMEM((6, width, width), f32),
            pltpu.VMEM((n, width, width), jnp.bfloat16),
            pltpu.VMEM((4, epochs, width), f32),
            pltpu.VMEM((epochs, n, width), f32),
            pltpu.VMEM((epochs, n, width), f32),
            pltpu.SemaphoreType.REGULAR((n,)),
            pltpu.SemaphoreType.DMA((3,)),
            pltpu.SemaphoreType.DMA((3, n)),
            pltpu.SemaphoreType.DMA((15,)),
        ]
    else:
        program = kernel
        scratch = [
            pltpu.VMEM((3, width), f32),
            pltpu.VMEM((3, width), f32),
            pltpu.VMEM((1, width), f32),
            pltpu.VMEM((1, width), f32),
            pltpu.VMEM((1, epochs), f32),
            pltpu.VMEM((1, n_samples), jnp.int32),
            pltpu.SMEM((1, occupancy.shape[1]), jnp.int32),
            pltpu.VMEM((n, 4, width), f32),
            pltpu.VMEM((n, 4, width), f32),
            pltpu.VMEM((3, n, width), f32),
            pltpu.VMEM((2 * n, width), f32),
            pltpu.VMEM((6, width, width), f32),
            pltpu.VMEM((n, width, width), jnp.bfloat16),
            pltpu.VMEM((epochs, width), f32),
            pltpu.VMEM((epochs, width), f32),
            pltpu.VMEM((epochs, width), f32),
            pltpu.VMEM((n, epochs // GROUP, GROUP, width), jnp.bfloat16),
            pltpu.SemaphoreType.DMA((6,)),
            pltpu.SemaphoreType.DMA((9,)),
        ]
    held = pl.pallas_call(
        functools.partial(program, n_recv, n_src),
        out_shape=(
            pltpu.VMEM((epochs, width), f32),
            pltpu.VMEM((epochs, width), f32),
            pltpu.VMEM((1, width), f32),
            pltpu.VMEM(soil.shape, f32),
        ),
        in_specs=[pl.BlockSpec(memory_space=pl.ANY)] * 9,
        out_specs=(vmem,) * 4,
        scratch_shapes=scratch,
        compiler_params=pltpu.CompilerParams(collective_id=0, has_side_effects=True),
    )(
        positions,
        normals,
        area.reshape(1, width),
        albedo.reshape(1, width),
        conductivity.reshape(1, width),
        soil,
        sun_tan.reshape(1, epochs),
        samples,
        occupancy,
    )
    return pl.pallas_call(
        conduct,
        out_shape=(
            jax.ShapeDtypeStruct(soil.shape, f32),
            jax.ShapeDtypeStruct((epochs, width), f32),
        ),
        in_specs=[vmem] * 4,
        out_specs=(vmem, vmem),
    )(*(pltpu.with_memory_space_constraint(value, pltpu.VMEM) for value in held))


def solution(mesh):
    in_specs = (
        P(None, ("basin", "recv", "src")),
        P(None, ("basin", "recv", "src")),
        P(("basin", "recv", "src")),
        P(("basin", "recv", "src")),
        P(("basin", "recv", "src")),
        P(None, ("basin", "recv", "src")),
        P(),
        P(("basin", "recv", "src"), None),
        P("basin", None),
    )
    out_specs = (P(None, ("basin", "recv", "src")), P(None, ("basin", "recv", "src")))
    return jax.shard_map(body, mesh=mesh, in_specs=in_specs, out_specs=out_specs, check_vma=False)
```

```python
import functools
import math

import jax
import jax.numpy as jnp
from jax import lax
from jax.experimental import pallas as pl
from jax.experimental.pallas import tpu as pltpu
from jax.sharding import PartitionSpec as P

solar_flux = 2.0
emissivity = 0.9
surface_gain = 0.1
shade_width = 0.1
reach_offset = 0.05
GROUP = 8
CHUNK = 16
TURNS = 32
PAIR = 2


def fourth(value):
    square = value * value
    return square * square


def column(row, count):
    wide = jnp.broadcast_to(row[:, :count], (count, count))
    here = lax.broadcasted_iota(jnp.int32, (count, count), 0) == lax.broadcasted_iota(
        jnp.int32, (count, count), 1
    )
    return jnp.sum(jnp.where(here, wide, 0.0), axis=1, keepdims=True)


def kernel(
    n_recv,
    n_src,
    pos_in,
    nrm_in,
    area_in,
    alb_in,
    cond_in,
    soil_in,
    tan_in,
    smp_in,
    occ_in,
    bounce_ref,
    heat_ref,
    cond_ref,
    soil_ref,
    pos_ref,
    nrm_ref,
    area_ref,
    alb_ref,
    tan_ref,
    smp_ref,
    occ_ref,
    near,
    far,
    planes,
    shifts,
    cols,
    view,
    direct_ref,
    lit_ref,
    tall_tan,
    radg,
    sems,
    loads,
):
    n = n_recv * n_src
    width = pos_ref.shape[1]
    n_samples = smp_ref.shape[1]
    epochs = tan_ref.shape[1]
    bits = width.bit_length() - 1
    few = n <= 16
    me = lax.axis_index("recv") * n_src + lax.axis_index("src")

    def peer(k):
        p = (me + (n - k)) & (n - 1)
        return {"recv": p >> (n_src.bit_length() - 1), "src": p & (n_src - 1)}

    def over(first, last, step):
        if few:
            for k in sorted(range(first, last), key=lambda k: abs(2 * k - n)):
                step(k)
        else:
            lax.fori_loop(first, last, lambda k, c: (step(k), c)[1], 0)

    barrier = pltpu.get_barrier_semaphore()
    over(
        1,
        n,
        lambda k: pl.semaphore_signal(
            barrier, inc=1, device_id=peer(k), device_id_type=pl.DeviceIdType.MESH
        ),
    )
    pairs = (
        (pos_in, pos_ref),
        (smp_in, smp_ref),
        (nrm_in, nrm_ref),
        (area_in, area_ref),
        (tan_in, tan_ref),
        (soil_in, soil_ref),
        (alb_in, alb_ref),
        (cond_in, cond_ref),
        (occ_in.at[pl.ds(me, 1)], occ_ref),
    )
    fetched = [
        pltpu.make_async_copy(there, here, loads.at[i]) for i, (there, here) in enumerate(pairs)
    ]
    for copy in fetched:
        copy.start()
    for copy in fetched[:4]:
        copy.wait()
    near[0, 0:3, :] = pos_ref[...]
    near[0, 3:4, 0:n_samples] = smp_ref[...].astype(jnp.float32)
    far[0, 0:3, :] = nrm_ref[...]
    far[0, 3:4, :] = area_ref[...]
    for copy in fetched[4:]:
        copy.wait()
    pl.semaphore_wait(barrier, n - 1)

    def send(ref, k, which):
        pltpu.make_async_remote_copy(
            src_ref=ref.at[0],
            dst_ref=ref.at[k],
            send_sem=sems.at[which],
            recv_sem=sems.at[which + 1],
            device_id=peer(k),
            device_id_type=pl.DeviceIdType.MESH,
        ).start()

    def everyone(ref, which):
        return pltpu.make_async_remote_copy(
            src_ref=ref.at[pl.ds(1, n - 1)],
            dst_ref=ref.at[pl.ds(1, n - 1)],
            send_sem=sems.at[which],
            recv_sem=sems.at[which + 1],
            device_id=peer(1),
            device_id_type=pl.DeviceIdType.MESH,
        )

    over(1, n, lambda k: send(near, k, 0))
    over(1, n, lambda k: send(far, k, 4))

    mine = near[0]
    tall = jnp.transpose(jnp.concatenate([mine, far[0]], axis=0))
    for c, at in enumerate((0, 1, 2, 4, 5, 6)):
        cols[c] = jnp.broadcast_to(tall[:, at : at + 1], (width, width))
    tan = column(tan_ref[...], epochs)
    angle = (
        2.0
        * math.pi
        * lax.broadcasted_iota(jnp.int32, (epochs, width), 0).astype(jnp.float32)
        / epochs
    )
    cos_e = 1.0 / jnp.sqrt(1.0 + tan * tan)
    incidence = (
        cos_e * jnp.cos(angle) * nrm_ref[0:1, :]
        + cos_e * jnp.sin(angle) * nrm_ref[1:2, :]
        + tan * cos_e * nrm_ref[2:3, :]
    )
    lit_ref[...] = solar_flux * jnp.maximum(incidence, 0.0)
    tall_tan[...] = jnp.broadcast_to(tan, (epochs, width))
    infrared = emissivity * fourth(soil_ref[0:1, :])

    everyone(near, 0).wait_recv()
    for c in range(3):
        planes[c] = near[:, c, :]
    rows = near[:, 3, :]
    shifts[0:n, :] = rows
    shifts[n : 2 * n, :] = rows

    lane = lax.broadcasted_iota(jnp.int32, (GROUP, width), 1)
    px, py, pz = (jnp.broadcast_to(mine[c : c + 1, :], (GROUP, width)) for c in range(3))

    def azimuths(group):
        offset = n - me + group * GROUP
        steps = shifts[pl.ds(offset, GROUP), :].astype(jnp.int32)
        best = jnp.full((GROUP, width), -1e30, jnp.float32)
        for s in range(n_samples):
            shift = jnp.broadcast_to(steps[:, s : s + 1], (GROUP, width))
            row = ((shift + (width - 1) - lane) >> bits) & (n - 1)
            within = row & (GROUP - 1)
            part = row >> (GROUP.bit_length() - 1)
            turn = (lane + shift) & (width - 1)
            found = []
            for c in range(3):
                picked = None
                for g in range(n // GROUP):
                    block = planes[c, g * GROUP : (g + 1) * GROUP, :]
                    got = jnp.take_along_axis(block, within, axis=0)
                    picked = got if picked is None else jnp.where(part == g, got, picked)
                found.append(jnp.take_along_axis(picked, turn, axis=1))
            dx = found[0] - px
            dy = found[1] - py
            reach = jnp.sqrt(dx * dx + dy * dy) + reach_offset
            best = jnp.maximum(best, (found[2] - pz) / reach)
        start = group * GROUP
        here = pl.ds(start if few else pl.multiple_of(start, GROUP), GROUP)
        direct = lit_ref[here, :] * jax.nn.sigmoid((tall_tan[here, :] - best) / shade_width)
        direct_ref[here, :] = direct
        radg[0, group] = (alb_ref[...] * direct + infrared).astype(jnp.bfloat16)
        over(1, n, lambda k: send(radg.at[:, group], k, 2))

    over(0, n // GROUP, azimuths)

    def see(k, carry):
        weight = occ_ref[0, lax.rem(me + k, n)].astype(jnp.float32)
        sx, sy, sz = (near[k, c : c + 1, :] for c in range(3))
        ox, oy, oz, size = (far[k, c : c + 1, :] for c in range(4))
        scale = size * weight / math.pi
        for i in range(width // CHUNK):
            at = slice(i * CHUNK, (i + 1) * CHUNK)
            dx = sx - cols[0, at, :]
            dy = sy - cols[1, at, :]
            dz = sz - cols[2, at, :]
            facing = cols[3, at, :] * dx + cols[4, at, :] * dy + cols[5, at, :] * dz
            toward = -(ox * dx + oy * dy + oz * dz)
            spread = dx * dx + dy * dy + dz * dz + size
            seen = jnp.maximum(facing, 0.0) * jnp.maximum(toward, 0.0) * scale
            view[k, at, :] = (seen / (spread * spread)).astype(jnp.bfloat16)
        return carry

    everyone(far, 4).wait_recv()
    lax.fori_loop(0, n, see, 0)
    everyone(radg, 2).wait_recv()

    def fold(k, total):
        sent = jnp.concatenate([radg[k, g] for g in range(epochs // GROUP)], axis=0)
        return total + lax.dot_general(
            sent, view[k], (((1,), (1,)), ((), ())), preferred_element_type=jnp.float32
        )

    total = jnp.zeros((epochs, width), jnp.float32)
    if few:
        for k in range(n):
            total = fold(k, total)
    else:
        total = lax.fori_loop(0, n, fold, total)
    bounce_ref[...] = total
    keep = surface_gain * (1.0 - alb_ref[...])
    heat_ref[...] = keep * (direct_ref[...] + total)
    everyone(near, 0).wait_send()
    everyone(far, 4).wait_send()
    everyone(radg, 2).wait_send()


def step(
    n_recv,
    n_src,
    pos_in,
    nrm_in,
    area_in,
    alb_in,
    cond_in,
    soil_in,
    tan_in,
    smp_in,
    occ_in,
    bounce_ref,
    heat_ref,
    cond_ref,
    soil_ref,
    tan_ref,
    occ_ref,
    facts,
    offsets,
    smp,
    planes,
    table,
    cols,
    view,
    sun_ref,
    direct_ref,
    lit_ref,
    hello,
    sent,
    got,
    loads,
):
    n = n_recv * n_src
    width = soil_ref.shape[1]
    n_samples = smp.shape[2]
    epochs = tan_ref.shape[1]
    bits = width.bit_length() - 1
    n_facts = facts.shape[0]
    chip_bits = n_src.bit_length() - 1
    quarter = n // 4
    pitch = 2 * n + 8
    me = lax.axis_index("recv") * n_src + lax.axis_index("src")
    chip = lax.axis_index("recv")

    def device(p):
        return {"recv": p >> chip_bits, "src": p & (n_src - 1)}

    def greet(sem, p):
        pl.semaphore_signal(sem, inc=1, device_id=device(p), device_id_type=pl.DeviceIdType.MESH)

    def each(first, last, do):
        lax.fori_loop(first, last, lambda p, c: (do(p), c)[1], 0)

    own = pl.ds(me, 1)
    fill = [(pos_in.at[pl.ds(c, 1)], facts.at[c, own]) for c in range(3)]
    fill += [(nrm_in.at[pl.ds(c, 1)], facts.at[3 + c, own]) for c in range(3)]
    fill += [(area_in, facts.at[6, own]), (alb_in, facts.at[7, own])]
    fill += [(soil_in.at[pl.ds(0, 1)], facts.at[8, own])]
    for there, here in fill:
        pltpu.make_async_copy(there, here, loads.at[0]).start()
    pairs = (
        (smp_in, offsets.at[me]),
        (tan_in, tan_ref),
        (soil_in, soil_ref),
        (cond_in, cond_ref),
        (occ_in.at[own], occ_ref),
    )
    fetched = [
        pltpu.make_async_copy(there, here, loads.at[1 + i]) for i, (there, here) in enumerate(pairs)
    ]
    for copy in fetched:
        copy.start()
    barrier = pltpu.get_barrier_semaphore()
    each(me + 1, n, lambda p: greet(barrier, p))
    pl.when(me > 0)(lambda: pl.semaphore_wait(barrier, me))
    each(0, me, lambda p: greet(hello.at[chip], p))

    def remote(slots, to, sem):
        return pltpu.make_async_remote_copy(
            src_ref=facts.at[:, slots],
            dst_ref=facts.at[:, slots],
            send_sem=sent.at[0],
            recv_sem=got.at[sem],
            device_id=device(to),
            device_id_type=pl.DeviceIdType.MESH,
        )

    def remote_offsets(slot, to):
        return pltpu.make_async_remote_copy(
            src_ref=offsets.at[slot],
            dst_ref=offsets.at[slot],
            send_sem=sent.at[1],
            recv_sem=got.at[n_recv],
            device_id=device(to),
            device_id_type=pl.DeviceIdType.MESH,
        )

    def tell(p):
        remote(own, p, chip).start()
        remote_offsets(me, p).start()

    pltpu.make_async_copy(facts.at[:, own], facts.at[:, own], loads.at[0]).wait()
    fetched[0].wait()
    each(0, me, tell)
    for copy in fetched[1:]:
        copy.wait()

    mine = jnp.concatenate([facts[0:6, me, :], facts[0:2, me, :]], axis=0)
    tall = jnp.transpose(mine)
    for c in range(6):
        cols[c] = jnp.broadcast_to(tall[:, c : c + 1], (width, width))
    tan = column(tan_ref[...], epochs)
    angle = (
        2.0
        * math.pi
        * lax.broadcasted_iota(jnp.int32, (epochs, width), 0).astype(jnp.float32)
        / epochs
    )
    cos_e = 1.0 / jnp.sqrt(1.0 + tan * tan)
    sun_ref[0] = cos_e * jnp.cos(angle)
    sun_ref[1] = cos_e * jnp.sin(angle)
    sun_ref[2] = jnp.broadcast_to(tan * cos_e, (epochs, width))
    sun_ref[3] = jnp.broadcast_to(tan, (epochs, width))

    def see(p):
        weight = occ_ref[0, p].astype(jnp.float32)
        row = pl.ds(p, 1)
        sx, sy, sz, ox, oy, oz, size = (facts[c, row, :] for c in range(7))
        scale = size * weight / math.pi
        for i in range(width // CHUNK):
            at = slice(i * CHUNK, (i + 1) * CHUNK)
            dx = sx - cols[0, at, :]
            dy = sy - cols[1, at, :]
            dz = sz - cols[2, at, :]
            facing = cols[3, at, :] * dx + cols[4, at, :] * dy + cols[5, at, :] * dz
            toward = -(ox * dx + oy * dy + oz * dz)
            spread = dx * dx + dy * dy + dz * dz + size
            seen = jnp.maximum(facing, 0.0) * jnp.maximum(toward, 0.0) * scale
            view[p, at, :] = (seen / (spread * spread)).astype(jnp.bfloat16)

    see(me)
    for other in range(1, n_src):
        p = me ^ other

        def answer_here():
            pl.semaphore_wait(hello.at[chip], 1)
            tell(p)

        pl.when(p > me)(answer_here)

    def answer(g):
        pl.semaphore_wait(hello.at[g], n_src)
        for core in range(n_src):
            tell(g * n_src + core)

    each(chip + 1, n_recv, answer)

    for other in range(1, n_src):
        remote(pl.ds(me ^ other, 1), me ^ other, chip).wait_recv()
        see(me ^ other)

    def arrive(m):
        g = chip ^ m
        remote(pl.ds(g * n_src, n_src), me ^ 1, g).wait_recv()

    def arrive_and_see(m):
        arrive(m)
        for core in range(n_src):
            see((chip ^ m) * n_src + core)

    late = n_recv - n_recv // 4
    each(1, late, arrive_and_see)

    def spread_rows():
        for c in range(3):
            planes[c, 0:8, :] = planes[c, n : n + 8, :]
            planes[c, n + 8 : n + 16, :] = planes[c, 8:16, :]

    def place(m):
        start = ((me // quarter) ^ m) * quarter
        for c in range(3):
            planes[c, pl.ds(8 + start, quarter), :] = facts[c, pl.ds(start, quarter), :]

    for m in range(3):
        place(m)
    gap = ((me // quarter) ^ 3) * quarter
    for c in range(3):
        planes[c, pl.ds(8 + gap, quarter), :] = jnp.zeros((quarter, width), jnp.float32)
    spread_rows()
    lane = lax.broadcasted_iota(jnp.int32, (8, width), 1)

    def turn(r, start, here, after):
        mixed = jnp.where(lane >= r, here, after)
        return pltpu.roll(mixed, (width - r) & (width - 1), 1)

    def spin(i, carry):
        for j in range(TURNS):
            r = i * TURNS + j
            for c in range(3):
                for g in range(n // 8):
                    at = 8 + g * 8
                    turned = turn(r, at, planes[c, at : at + 8, :], planes[c, at + 1 : at + 9, :])
                    table[c, pl.ds(r * pitch + at, 8), :] = turned
                    table[c, pl.ds(r * pitch + at + n, 8), :] = turned
        return carry

    lax.fori_loop(0, width // TURNS, spin, 0)
    each(late, n_recv, arrive)
    remote_everything = pltpu.make_async_remote_copy(
        src_ref=offsets.at[pl.ds(0, n - 1)],
        dst_ref=offsets.at[pl.ds(0, n - 1)],
        send_sem=sent.at[1],
        recv_sem=got.at[n_recv],
        device_id=device(me ^ 1),
        device_id_type=pl.DeviceIdType.MESH,
    )
    remote_everything.wait_recv()
    scalars = pltpu.make_async_copy(offsets, smp, loads.at[6])
    scalars.start()
    place(3)
    spread_rows()

    def respin(i, carry):
        at = 7 + gap
        for j in range(width // quarter):
            r = i * (width // quarter) + j
            for c in range(3):
                here = planes[c, pl.ds(at, 8), :]
                after = planes[c, pl.ds(at + 1, 8), :]
                turned = turn(r, at, here, after)
                table[c, pl.ds(r * pitch + at, 8), :] = turned
                table[c, pl.ds(r * pitch + at + n, 8), :] = turned
        see(gap + i)
        return carry

    lax.fori_loop(0, quarter, respin, 0)
    scalars.wait()

    def horizon(a):
        here = [[planes[c, 8 + g * 8 : 16 + g * 8, :] for g in range(n // 8)] for c in range(3)]
        best = [jnp.full((8, width), -1e30, jnp.float32) for g in range(n // 8)]
        for s in range(n_samples):
            shift = smp[a, 0, s]
            start = (shift & (width - 1)) * pitch + (shift >> bits) + 8
            for g in range(n // 8):
                fx, fy, fz = (table[c, pl.ds(start + g * 8, 8), :] for c in range(3))
                dx = fx - here[0][g]
                dy = fy - here[1][g]
                square = jnp.maximum(dx * dx + dy * dy, 1e-30)
                reach = square * lax.rsqrt(square) + reach_offset
                best[g] = jnp.maximum(best[g], (fz - here[2][g]) / reach)
        line = pl.ds(a, 1)
        cx, cy, cz, tans = (sun_ref[c, line, :] for c in range(4))
        for g in range(n // 8):
            at = slice(g * 8, g * 8 + 8)
            incidence = cx * facts[3, at, :] + cy * facts[4, at, :] + cz * facts[5, at, :]
            shade = jax.nn.sigmoid((tans - best[g]) / shade_width)
            direct = solar_flux * jnp.maximum(incidence, 0.0) * shade
            direct_ref[a, at, :] = direct
            lit_ref[a, at, :] = facts[7, at, :] * direct + emissivity * fourth(facts[8, at, :])

    def horizons(i, carry):
        for j in range(PAIR):
            horizon(i * PAIR + j)
        return carry

    lax.fori_loop(0, epochs // PAIR, horizons, 0)

    total = jnp.zeros((epochs, width), jnp.float32)
    for p in range(n):
        total = total + lax.dot_general(
            lit_ref[:, p, :].astype(jnp.bfloat16),
            view[p],
            (((1,), (1,)), ((), ())),
            preferred_element_type=jnp.float32,
        )
    bounce_ref[...] = total
    keep = surface_gain * (1.0 - facts[7, own, :])
    heat_ref[...] = keep * (direct_ref[:, me, :] + total)
    remote(pl.ds(0, n - 1), me ^ 1, 0).wait_send()
    remote_everything.wait_send()


def conduct(bounce_in, heat_ref, cond_ref, soil_ref, final_ref, bounce_ref):
    layers, width = soil_ref.shape
    epochs = heat_ref.shape[0]
    bounce_ref[...] = bounce_in[...]
    cond = cond_ref[...]
    first = lax.broadcasted_iota(jnp.int32, (layers, width), 0) == 0
    last = lax.broadcasted_iota(jnp.int32, (layers, width), 0) == layers - 1

    def advance(t, temps):
        below = jnp.where(last, temps, pltpu.roll(temps, layers - 1, 0))
        above = jnp.where(first, temps, pltpu.roll(temps, 1, 0))
        temps = temps + cond * ((below - temps) - (temps - above))
        gain = heat_ref[pl.ds(t, 1), :] - (surface_gain * emissivity) * fourth(temps)
        return jnp.where(first, temps + gain, temps)

    temps = soil_ref[...]
    if epochs <= 16:
        for t in range(epochs):
            temps = advance(t, temps)
    else:
        temps = lax.fori_loop(0, epochs, advance, temps)
    final_ref[...] = temps


def body(positions, normals, area, albedo, conductivity, soil, sun_tan, samples, occupancy):
    n_recv = lax.axis_size("recv")
    n_src = lax.axis_size("src")
    n = n_recv * n_src
    width = positions.shape[1]
    epochs = sun_tan.shape[0]
    vmem = pl.BlockSpec(memory_space=pltpu.VMEM)
    f32 = jnp.float32
    n_samples = samples.shape[1]
    if n <= 16:
        program = step
        scratch = [
            pltpu.VMEM((1, epochs), f32),
            pltpu.SMEM((1, occupancy.shape[1]), jnp.int32),
            pltpu.VMEM((9, n, width), f32),
            pltpu.VMEM((n, 1, n_samples), jnp.int32),
            pltpu.SMEM((n, 1, n_samples), jnp.int32),
            pltpu.VMEM((3, n + 16, width), f32),
            pltpu.VMEM((3, width * (2 * n + 8) + 8, width), f32),
            pltpu.VMEM((6, width, width), f32),
            pltpu.VMEM((n, width, width), jnp.bfloat16),
            pltpu.VMEM((4, epochs, width), f32),
            pltpu.VMEM((epochs, n, width), f32),
            pltpu.VMEM((epochs, n, width), f32),
            pltpu.SemaphoreType.REGULAR((n_recv,)),
            pltpu.SemaphoreType.DMA((2,)),
            pltpu.SemaphoreType.DMA((n_recv + 1,)),
            pltpu.SemaphoreType.DMA((7,)),
        ]
    else:
        program = kernel
        scratch = [
            pltpu.VMEM((3, width), f32),
            pltpu.VMEM((3, width), f32),
            pltpu.VMEM((1, width), f32),
            pltpu.VMEM((1, width), f32),
            pltpu.VMEM((1, epochs), f32),
            pltpu.VMEM((1, n_samples), jnp.int32),
            pltpu.SMEM((1, occupancy.shape[1]), jnp.int32),
            pltpu.VMEM((n, 4, width), f32),
            pltpu.VMEM((n, 4, width), f32),
            pltpu.VMEM((3, n, width), f32),
            pltpu.VMEM((2 * n, width), f32),
            pltpu.VMEM((6, width, width), f32),
            pltpu.VMEM((n, width, width), jnp.bfloat16),
            pltpu.VMEM((epochs, width), f32),
            pltpu.VMEM((epochs, width), f32),
            pltpu.VMEM((epochs, width), f32),
            pltpu.VMEM((n, epochs // GROUP, GROUP, width), jnp.bfloat16),
            pltpu.SemaphoreType.DMA((6,)),
            pltpu.SemaphoreType.DMA((9,)),
        ]
    held = pl.pallas_call(
        functools.partial(program, n_recv, n_src),
        out_shape=(
            pltpu.VMEM((epochs, width), f32),
            pltpu.VMEM((epochs, width), f32),
            pltpu.VMEM((1, width), f32),
            pltpu.VMEM(soil.shape, f32),
        ),
        in_specs=[pl.BlockSpec(memory_space=pl.ANY)] * 9,
        out_specs=(vmem,) * 4,
        scratch_shapes=scratch,
        compiler_params=pltpu.CompilerParams(collective_id=0, has_side_effects=True),
    )(
        positions,
        normals,
        area.reshape(1, width),
        albedo.reshape(1, width),
        conductivity.reshape(1, width),
        soil,
        sun_tan.reshape(1, epochs),
        samples,
        occupancy,
    )
    return pl.pallas_call(
        conduct,
        out_shape=(
            jax.ShapeDtypeStruct(soil.shape, f32),
            jax.ShapeDtypeStruct((epochs, width), f32),
        ),
        in_specs=[vmem] * 4,
        out_specs=(vmem, vmem),
    )(*(pltpu.with_memory_space_constraint(value, pltpu.VMEM) for value in held))


def solution(mesh):
    in_specs = (
        P(None, ("basin", "recv", "src")),
        P(None, ("basin", "recv", "src")),
        P(("basin", "recv", "src")),
        P(("basin", "recv", "src")),
        P(("basin", "recv", "src")),
        P(None, ("basin", "recv", "src")),
        P(),
        P(("basin", "recv", "src"), None),
        P("basin", None),
    )
    out_specs = (P(None, ("basin", "recv", "src")), P(None, ("basin", "recv", "src")))
    return jax.shard_map(body, mesh=mesh, in_specs=in_specs, out_specs=out_specs, check_vma=False)
```

```python
import functools
import math

import jax
import jax.numpy as jnp
from jax import lax
from jax.experimental import pallas as pl
from jax.experimental.pallas import tpu as pltpu
from jax.sharding import PartitionSpec as P

solar_flux = 2.0
emissivity = 0.9
surface_gain = 0.1
shade_width = 0.1
reach_offset = 0.05
GROUP = 8
CHUNK = 16
TURNS = 32
PATCH = 64
PAIR = 4


def fourth(value):
    square = value * value
    return square * square


def column(row, count):
    wide = jnp.broadcast_to(row[:, :count], (count, count))
    here = lax.broadcasted_iota(jnp.int32, (count, count), 0) == lax.broadcasted_iota(
        jnp.int32, (count, count), 1
    )
    return jnp.sum(jnp.where(here, wide, 0.0), axis=1, keepdims=True)


def kernel(
    n_recv,
    n_src,
    pos_in,
    nrm_in,
    area_in,
    alb_in,
    cond_in,
    soil_in,
    tan_in,
    smp_in,
    occ_in,
    bounce_ref,
    heat_ref,
    cond_ref,
    soil_ref,
    pos_ref,
    nrm_ref,
    area_ref,
    alb_ref,
    tan_ref,
    smp_ref,
    occ_ref,
    near,
    far,
    planes,
    shifts,
    cols,
    view,
    direct_ref,
    lit_ref,
    tall_tan,
    radg,
    sems,
    loads,
):
    n = n_recv * n_src
    width = pos_ref.shape[1]
    n_samples = smp_ref.shape[1]
    epochs = tan_ref.shape[1]
    bits = width.bit_length() - 1
    few = n <= 16
    me = lax.axis_index("recv") * n_src + lax.axis_index("src")

    def peer(k):
        p = (me + (n - k)) & (n - 1)
        return {"recv": p >> (n_src.bit_length() - 1), "src": p & (n_src - 1)}

    def over(first, last, step):
        if few:
            for k in sorted(range(first, last), key=lambda k: abs(2 * k - n)):
                step(k)
        else:
            lax.fori_loop(first, last, lambda k, c: (step(k), c)[1], 0)

    barrier = pltpu.get_barrier_semaphore()
    over(
        1,
        n,
        lambda k: pl.semaphore_signal(
            barrier, inc=1, device_id=peer(k), device_id_type=pl.DeviceIdType.MESH
        ),
    )
    pairs = (
        (pos_in, pos_ref),
        (smp_in, smp_ref),
        (nrm_in, nrm_ref),
        (area_in, area_ref),
        (tan_in, tan_ref),
        (soil_in, soil_ref),
        (alb_in, alb_ref),
        (cond_in, cond_ref),
        (occ_in.at[pl.ds(me, 1)], occ_ref),
    )
    fetched = [
        pltpu.make_async_copy(there, here, loads.at[i]) for i, (there, here) in enumerate(pairs)
    ]
    for copy in fetched:
        copy.start()
    for copy in fetched[:4]:
        copy.wait()
    near[0, 0:3, :] = pos_ref[...]
    near[0, 3:4, 0:n_samples] = smp_ref[...].astype(jnp.float32)
    far[0, 0:3, :] = nrm_ref[...]
    far[0, 3:4, :] = area_ref[...]
    for copy in fetched[4:]:
        copy.wait()
    pl.semaphore_wait(barrier, n - 1)

    def send(ref, k, which):
        pltpu.make_async_remote_copy(
            src_ref=ref.at[0],
            dst_ref=ref.at[k],
            send_sem=sems.at[which],
            recv_sem=sems.at[which + 1],
            device_id=peer(k),
            device_id_type=pl.DeviceIdType.MESH,
        ).start()

    def everyone(ref, which):
        return pltpu.make_async_remote_copy(
            src_ref=ref.at[pl.ds(1, n - 1)],
            dst_ref=ref.at[pl.ds(1, n - 1)],
            send_sem=sems.at[which],
            recv_sem=sems.at[which + 1],
            device_id=peer(1),
            device_id_type=pl.DeviceIdType.MESH,
        )

    over(1, n, lambda k: send(near, k, 0))
    over(1, n, lambda k: send(far, k, 4))

    mine = near[0]
    tall = jnp.transpose(jnp.concatenate([mine, far[0]], axis=0))
    for c, at in enumerate((0, 1, 2, 4, 5, 6)):
        cols[c] = jnp.broadcast_to(tall[:, at : at + 1], (width, width))
    tan = column(tan_ref[...], epochs)
    angle = (
        2.0
        * math.pi
        * lax.broadcasted_iota(jnp.int32, (epochs, width), 0).astype(jnp.float32)
        / epochs
    )
    cos_e = 1.0 / jnp.sqrt(1.0 + tan * tan)
    incidence = (
        cos_e * jnp.cos(angle) * nrm_ref[0:1, :]
        + cos_e * jnp.sin(angle) * nrm_ref[1:2, :]
        + tan * cos_e * nrm_ref[2:3, :]
    )
    lit_ref[...] = solar_flux * jnp.maximum(incidence, 0.0)
    tall_tan[...] = jnp.broadcast_to(tan, (epochs, width))
    infrared = emissivity * fourth(soil_ref[0:1, :])

    everyone(near, 0).wait_recv()
    for c in range(3):
        planes[c] = near[:, c, :]
    rows = near[:, 3, :]
    shifts[0:n, :] = rows
    shifts[n : 2 * n, :] = rows

    lane = lax.broadcasted_iota(jnp.int32, (GROUP, width), 1)
    px, py, pz = (jnp.broadcast_to(mine[c : c + 1, :], (GROUP, width)) for c in range(3))

    def azimuths(group):
        offset = n - me + group * GROUP
        steps = shifts[pl.ds(offset, GROUP), :].astype(jnp.int32)
        best = jnp.full((GROUP, width), -1e30, jnp.float32)
        for s in range(n_samples):
            shift = jnp.broadcast_to(steps[:, s : s + 1], (GROUP, width))
            row = ((shift + (width - 1) - lane) >> bits) & (n - 1)
            within = row & (GROUP - 1)
            part = row >> (GROUP.bit_length() - 1)
            turn = (lane + shift) & (width - 1)
            found = []
            for c in range(3):
                picked = None
                for g in range(n // GROUP):
                    block = planes[c, g * GROUP : (g + 1) * GROUP, :]
                    got = jnp.take_along_axis(block, within, axis=0)
                    picked = got if picked is None else jnp.where(part == g, got, picked)
                found.append(jnp.take_along_axis(picked, turn, axis=1))
            dx = found[0] - px
            dy = found[1] - py
            reach = jnp.sqrt(dx * dx + dy * dy) + reach_offset
            best = jnp.maximum(best, (found[2] - pz) / reach)
        start = group * GROUP
        here = pl.ds(start if few else pl.multiple_of(start, GROUP), GROUP)
        direct = lit_ref[here, :] * jax.nn.sigmoid((tall_tan[here, :] - best) / shade_width)
        direct_ref[here, :] = direct
        radg[0, group] = (alb_ref[...] * direct + infrared).astype(jnp.bfloat16)
        over(1, n, lambda k: send(radg.at[:, group], k, 2))

    over(0, n // GROUP, azimuths)

    def see(k, carry):
        weight = occ_ref[0, lax.rem(me + k, n)].astype(jnp.float32)
        sx, sy, sz = (near[k, c : c + 1, :] for c in range(3))
        ox, oy, oz, size = (far[k, c : c + 1, :] for c in range(4))
        scale = size * weight / math.pi
        for i in range(width // CHUNK):
            at = slice(i * CHUNK, (i + 1) * CHUNK)
            dx = sx - cols[0, at, :]
            dy = sy - cols[1, at, :]
            dz = sz - cols[2, at, :]
            facing = cols[3, at, :] * dx + cols[4, at, :] * dy + cols[5, at, :] * dz
            toward = -(ox * dx + oy * dy + oz * dz)
            spread = dx * dx + dy * dy + dz * dz + size
            seen = jnp.maximum(facing, 0.0) * jnp.maximum(toward, 0.0) * scale
            view[k, at, :] = (seen / (spread * spread)).astype(jnp.bfloat16)
        return carry

    everyone(far, 4).wait_recv()
    lax.fori_loop(0, n, see, 0)
    everyone(radg, 2).wait_recv()

    def fold(k, total):
        sent = jnp.concatenate([radg[k, g] for g in range(epochs // GROUP)], axis=0)
        return total + lax.dot_general(
            sent, view[k], (((1,), (1,)), ((), ())), preferred_element_type=jnp.float32
        )

    total = jnp.zeros((epochs, width), jnp.float32)
    if few:
        for k in range(n):
            total = fold(k, total)
    else:
        total = lax.fori_loop(0, n, fold, total)
    bounce_ref[...] = total
    keep = surface_gain * (1.0 - alb_ref[...])
    heat_ref[...] = keep * (direct_ref[...] + total)
    everyone(near, 0).wait_send()
    everyone(far, 4).wait_send()
    everyone(radg, 2).wait_send()


def step(
    n_recv,
    n_src,
    pos_in,
    nrm_in,
    area_in,
    alb_in,
    cond_in,
    soil_in,
    tan_in,
    smp_in,
    occ_in,
    bounce_ref,
    heat_ref,
    cond_ref,
    soil_ref,
    tan_ref,
    occ_ref,
    facts,
    offsets,
    smp,
    planes,
    table,
    cols,
    view,
    sun_ref,
    direct_ref,
    lit_ref,
    hello,
    sent,
    got,
    loads,
):
    n = n_recv * n_src
    width = soil_ref.shape[1]
    n_samples = smp.shape[2]
    epochs = tan_ref.shape[1]
    bits = width.bit_length() - 1
    n_facts = facts.shape[0]
    chip_bits = n_src.bit_length() - 1
    quarter = n // 4
    pitch = 2 * n + 8
    me = lax.axis_index("recv") * n_src + lax.axis_index("src")
    chip = lax.axis_index("recv")

    def device(p):
        return {"recv": p >> chip_bits, "src": p & (n_src - 1)}

    def greet(sem, p):
        pl.semaphore_signal(sem, inc=1, device_id=device(p), device_id_type=pl.DeviceIdType.MESH)

    def each(first, last, do):
        lax.fori_loop(first, last, lambda p, c: (do(p), c)[1], 0)

    own = pl.ds(me, 1)
    fill = [(pos_in.at[pl.ds(c, 1)], facts.at[c, own]) for c in range(3)]
    fill += [(nrm_in.at[pl.ds(c, 1)], facts.at[3 + c, own]) for c in range(3)]
    fill += [(area_in, facts.at[6, own]), (alb_in, facts.at[7, own])]
    fill += [(soil_in.at[pl.ds(0, 1)], facts.at[8, own])]
    for there, here in fill:
        pltpu.make_async_copy(there, here, loads.at[0]).start()
    pairs = (
        (smp_in, offsets.at[me]),
        (tan_in, tan_ref),
        (soil_in, soil_ref),
        (cond_in, cond_ref),
        (occ_in.at[own], occ_ref),
    )
    fetched = [
        pltpu.make_async_copy(there, here, loads.at[1 + i]) for i, (there, here) in enumerate(pairs)
    ]
    for copy in fetched:
        copy.start()
    barrier = pltpu.get_barrier_semaphore()
    each(me + 1, n, lambda p: greet(barrier, p))
    pl.when(me > 0)(lambda: pl.semaphore_wait(barrier, me))
    each(0, me, lambda p: greet(hello.at[chip], p))

    def remote(slots, to, sem):
        return pltpu.make_async_remote_copy(
            src_ref=facts.at[:, slots],
            dst_ref=facts.at[:, slots],
            send_sem=sent.at[0],
            recv_sem=got.at[sem],
            device_id=device(to),
            device_id_type=pl.DeviceIdType.MESH,
        )

    def remote_offsets(slot, to):
        return pltpu.make_async_remote_copy(
            src_ref=offsets.at[slot],
            dst_ref=offsets.at[slot],
            send_sem=sent.at[1],
            recv_sem=got.at[n_recv + slot // quarter],
            device_id=device(to),
            device_id_type=pl.DeviceIdType.MESH,
        )

    def tell(p):
        remote(own, p, chip).start()
        remote_offsets(me, p).start()

    pltpu.make_async_copy(facts.at[:, own], facts.at[:, own], loads.at[0]).wait()
    fetched[0].wait()
    each(0, me, tell)
    for copy in fetched[1:]:
        copy.wait()

    mine = jnp.concatenate([facts[0:6, me, :], facts[0:2, me, :]], axis=0)
    tall = jnp.transpose(mine)
    for c in range(6):
        cols[c] = jnp.broadcast_to(tall[:, c : c + 1], (width, width))
    tan = column(tan_ref[...], epochs)
    angle = (
        2.0
        * math.pi
        * lax.broadcasted_iota(jnp.int32, (epochs, width), 0).astype(jnp.float32)
        / epochs
    )
    cos_e = 1.0 / jnp.sqrt(1.0 + tan * tan)
    sun_ref[0] = cos_e * jnp.cos(angle)
    sun_ref[1] = cos_e * jnp.sin(angle)
    sun_ref[2] = jnp.broadcast_to(tan * cos_e, (epochs, width))
    sun_ref[3] = jnp.broadcast_to(tan, (epochs, width))

    def glimpses(p):
        weight = occ_ref[0, p].astype(jnp.float32)
        row = pl.ds(p, 1)
        sx, sy, sz, ox, oy, oz, size = (facts[c, row, :] for c in range(7))
        scale = size * weight / math.pi

        def glimpse(i):
            at = slice(i * CHUNK, (i + 1) * CHUNK)
            dx = sx - cols[0, at, :]
            dy = sy - cols[1, at, :]
            dz = sz - cols[2, at, :]
            facing = cols[3, at, :] * dx + cols[4, at, :] * dy + cols[5, at, :] * dz
            toward = -(ox * dx + oy * dy + oz * dz)
            spread = dx * dx + dy * dy + dz * dz + size
            seen = jnp.maximum(facing, 0.0) * jnp.maximum(toward, 0.0) * scale
            view[p, at, :] = (seen / (spread * spread)).astype(jnp.bfloat16)

        return [functools.partial(glimpse, i) for i in range(width // CHUNK)]

    def see(p):
        for glimpse in glimpses(p):
            glimpse()

    see(me)
    for other in range(1, n_src):
        p = me ^ other

        def answer_here():
            pl.semaphore_wait(hello.at[chip], 1)
            tell(p)

        pl.when(p > me)(answer_here)

    def answer(g):
        pl.semaphore_wait(hello.at[g], n_src)
        for core in range(n_src):
            tell(g * n_src + core)

    each(chip + 1, n_recv, answer)

    for other in range(1, n_src):
        remote(pl.ds(me ^ other, 1), me ^ other, chip).wait_recv()
        see(me ^ other)

    def arrive(m):
        g = chip ^ m
        remote(pl.ds(g * n_src, n_src), me ^ 1, g).wait_recv()

    def arrive_and_see(m):
        arrive(m)
        for core in range(n_src):
            see((chip ^ m) * n_src + core)

    late = n_recv - n_recv // 4
    each(1, late, arrive_and_see)

    def spread_rows():
        for c in range(3):
            planes[c, 0:8, :] = planes[c, n : n + 8, :]
            planes[c, n + 8 : n + 16, :] = planes[c, 8:16, :]

    def place(m):
        start = ((me // quarter) ^ m) * quarter
        for c in range(3):
            planes[c, pl.ds(8 + start, quarter), :] = facts[c, pl.ds(start, quarter), :]

    for m in range(3):
        place(m)
    gap = ((me // quarter) ^ 3) * quarter
    for c in range(3):
        planes[c, pl.ds(8 + gap, quarter), :] = jnp.zeros((quarter, width), jnp.float32)
    spread_rows()
    lane = lax.broadcasted_iota(jnp.int32, (8, width), 1)

    def turn(r, here, after):
        mixed = jnp.where(lane >= r, here, after)
        return pltpu.roll(mixed, (width - r) & (width - 1), 1)

    def spin(i, carry):
        for j in range(TURNS):
            r = i * TURNS + j
            for c in range(3):
                for g in range(n // 8):
                    at = 8 + g * 8
                    turned = turn(r, planes[c, at : at + 8, :], planes[c, at + 1 : at + 9, :])
                    table[c, pl.ds(r * pitch + at, 8), :] = turned
                    table[c, pl.ds(r * pitch + at + n, 8), :] = turned
        return carry

    def samples_of(m, count):
        slots = pl.ds(0, count)
        return pltpu.make_async_remote_copy(
            src_ref=offsets.at[slots],
            dst_ref=offsets.at[slots],
            send_sem=sent.at[1],
            recv_sem=got.at[n_recv + ((me // quarter) ^ m)],
            device_id=device(me ^ 1),
            device_id_type=pl.DeviceIdType.MESH,
        )

    def to_scalars(m):
        slots = pl.ds(((me // quarter) ^ m) * quarter, quarter)
        return pltpu.make_async_copy(offsets.at[slots], smp.at[slots], loads.at[6 + m])

    for m in range(3):
        samples_of(m, quarter - (m == 0)).wait_recv()
        to_scalars(m).start()
    lax.fori_loop(0, width // TURNS, spin, 0)
    each(late, n_recv, arrive)
    samples_of(3, quarter).wait_recv()
    to_scalars(3).start()
    place(3)
    spread_rows()

    at = 7 + gap
    window = [[planes[c, pl.ds(at + k, 8), :] for k in range(2)] for c in range(3)]

    def respin(i, carry):
        blocks = quarter * PATCH // width
        todo = [g for j in range(blocks) for g in glimpses(gap + i * blocks + j)]
        for j in range(PATCH):
            r = i * PATCH + j
            for c in range(3):
                turned = turn(r, window[c][0], window[c][1])
                table[c, pl.ds(r * pitch + at, 8), :] = turned
                table[c, pl.ds(r * pitch + at + n, 8), :] = turned
            if j % (PATCH // len(todo)) == 0:
                todo[j // (PATCH // len(todo))]()
        return carry

    lax.fori_loop(0, width // PATCH, respin, 0)
    for m in range(3):
        to_scalars(m).wait()

    def horizon(a):
        here = [[planes[c, 8 + g * 8 : 16 + g * 8, :] for g in range(n // 8)] for c in range(3)]
        best = [jnp.full((8, width), -1e30, jnp.float32) for g in range(n // 8)]
        for s in range(n_samples):
            shift = smp[a, 0, s]
            start = (shift & (width - 1)) * pitch + (shift >> bits) + 8
            for g in range(n // 8):
                fx, fy, fz = (table[c, pl.ds(start + g * 8, 8), :] for c in range(3))
                dx = fx - here[0][g]
                dy = fy - here[1][g]
                reach = 1.0 / lax.rsqrt(dx * dx + dy * dy) + reach_offset
                best[g] = jnp.maximum(best[g], (fz - here[2][g]) / reach)
        line = pl.ds(a, 1)
        cx, cy, cz, tans = (sun_ref[c, line, :] for c in range(4))
        for g in range(n // 8):
            at = slice(g * 8, g * 8 + 8)
            incidence = cx * facts[3, at, :] + cy * facts[4, at, :] + cz * facts[5, at, :]
            shade = jax.nn.sigmoid((tans - best[g]) / shade_width)
            direct = solar_flux * jnp.maximum(incidence, 0.0) * shade
            put = pl.ds(pl.multiple_of(a * n + g * 8, 8), 8)
            direct_ref[put, :] = direct
            lit_ref[put, :] = facts[7, at, :] * direct + emissivity * fourth(facts[8, at, :])

    shared = epochs // 4
    core = me & 1
    partner = me ^ 1

    def azimuth(order):
        return ((me // quarter) ^ (order // quarter)) * quarter + (order & (quarter - 1))

    def swap(ref, which):
        return pltpu.make_async_remote_copy(
            src_ref=ref,
            dst_ref=ref,
            send_sem=sent.at[2 + which],
            recv_sem=got.at[n_recv + 4 + which],
            device_id=device(partner),
            device_id_type=pl.DeviceIdType.MESH,
        )

    def swaps(first, facet):
        start = pl.multiple_of(azimuth(first) * n, 8)
        lines = [direct_ref.at[pl.ds(start + k * n + facet, 1)] for k in range(shared)]
        return [swap(lit_ref.at[pl.ds(start, shared * n)], 0)] + [swap(line, 1) for line in lines]

    swapped = (swap(lit_ref.at[pl.ds(0, shared * n)], 0), swap(direct_ref.at[pl.ds(0, shared)], 1))

    def horizons(i, carry):
        @pl.when(i == shared // PAIR)
        def _():
            for copy in swaps(core * shared, partner):
                copy.start()

        @pl.when(i == 2 * shared // PAIR)
        def _():
            to_scalars(3).wait()

        first = jnp.where(i < shared // PAIR, core * shared, shared) + i * PAIR
        for j in range(PAIR):
            horizon(azimuth(first + j))
        return carry

    lax.fori_loop(0, 3 * shared // PAIR, horizons, 0)
    for copy in swapped:
        copy.wait_recv()

    total = jnp.zeros((epochs, width), jnp.float32)
    for p in range(n):
        total = total + lax.dot_general(
            lit_ref[pl.ds(p, epochs, stride=n), :].astype(jnp.bfloat16),
            view[p],
            (((1,), (1,)), ((), ())),
            preferred_element_type=jnp.float32,
        )
    bounce_ref[...] = total
    keep = surface_gain * (1.0 - facts[7, own, :])
    heat_ref[...] = keep * (direct_ref[pl.ds(me, epochs, stride=n), :] + total)
    remote(pl.ds(0, n - 1), me ^ 1, 0).wait_send()
    samples_of(0, n - 1).wait_send()
    for copy in swapped:
        copy.wait_send()


def conduct(bounce_in, heat_ref, cond_ref, soil_ref, final_ref, bounce_ref):
    layers, width = soil_ref.shape
    epochs = heat_ref.shape[0]
    bounce_ref[...] = bounce_in[...]
    cond = cond_ref[...]
    first = lax.broadcasted_iota(jnp.int32, (layers, width), 0) == 0
    last = lax.broadcasted_iota(jnp.int32, (layers, width), 0) == layers - 1

    def advance(t, temps):
        below = jnp.where(last, temps, pltpu.roll(temps, layers - 1, 0))
        above = jnp.where(first, temps, pltpu.roll(temps, 1, 0))
        temps = temps + cond * ((below - temps) - (temps - above))
        gain = heat_ref[pl.ds(t, 1), :] - (surface_gain * emissivity) * fourth(temps)
        return jnp.where(first, temps + gain, temps)

    temps = soil_ref[...]
    if epochs <= 16:
        for t in range(epochs):
            temps = advance(t, temps)
    else:
        temps = lax.fori_loop(0, epochs, advance, temps)
    final_ref[...] = temps


def body(positions, normals, area, albedo, conductivity, soil, sun_tan, samples, occupancy):
    n_recv = lax.axis_size("recv")
    n_src = lax.axis_size("src")
    n = n_recv * n_src
    width = positions.shape[1]
    epochs = sun_tan.shape[0]
    vmem = pl.BlockSpec(memory_space=pltpu.VMEM)
    f32 = jnp.float32
    n_samples = samples.shape[1]
    if n <= 16:
        program = step
        scratch = [
            pltpu.VMEM((1, epochs), f32),
            pltpu.SMEM((1, occupancy.shape[1]), jnp.int32),
            pltpu.VMEM((9, n, width), f32),
            pltpu.VMEM((n, 1, n_samples), jnp.int32),
            pltpu.SMEM((n, 1, n_samples), jnp.int32),
            pltpu.VMEM((3, n + 16, width), f32),
            pltpu.VMEM((3, width * (2 * n + 8) + 8, width), f32),
            pltpu.VMEM((6, width, width), f32),
            pltpu.VMEM((n, width, width), jnp.bfloat16),
            pltpu.VMEM((4, epochs, width), f32),
            pltpu.VMEM((epochs * n, width), f32),
            pltpu.VMEM((epochs * n, width), f32),
            pltpu.SemaphoreType.REGULAR((n_recv,)),
            pltpu.SemaphoreType.DMA((4,)),
            pltpu.SemaphoreType.DMA((n_recv + 6,)),
            pltpu.SemaphoreType.DMA((10,)),
        ]
    else:
        program = kernel
        scratch = [
            pltpu.VMEM((3, width), f32),
            pltpu.VMEM((3, width), f32),
            pltpu.VMEM((1, width), f32),
            pltpu.VMEM((1, width), f32),
            pltpu.VMEM((1, epochs), f32),
            pltpu.VMEM((1, n_samples), jnp.int32),
            pltpu.SMEM((1, occupancy.shape[1]), jnp.int32),
            pltpu.VMEM((n, 4, width), f32),
            pltpu.VMEM((n, 4, width), f32),
            pltpu.VMEM((3, n, width), f32),
            pltpu.VMEM((2 * n, width), f32),
            pltpu.VMEM((6, width, width), f32),
            pltpu.VMEM((n, width, width), jnp.bfloat16),
            pltpu.VMEM((epochs, width), f32),
            pltpu.VMEM((epochs, width), f32),
            pltpu.VMEM((epochs, width), f32),
            pltpu.VMEM((n, epochs // GROUP, GROUP, width), jnp.bfloat16),
            pltpu.SemaphoreType.DMA((6,)),
            pltpu.SemaphoreType.DMA((9,)),
        ]
    held = pl.pallas_call(
        functools.partial(program, n_recv, n_src),
        out_shape=(
            pltpu.VMEM((epochs, width), f32),
            pltpu.VMEM((epochs, width), f32),
            pltpu.VMEM((1, width), f32),
            pltpu.VMEM(soil.shape, f32),
        ),
        in_specs=[pl.BlockSpec(memory_space=pl.ANY)] * 9,
        out_specs=(vmem,) * 4,
        scratch_shapes=scratch,
        compiler_params=pltpu.CompilerParams(collective_id=0, has_side_effects=True),
    )(
        positions,
        normals,
        area.reshape(1, width),
        albedo.reshape(1, width),
        conductivity.reshape(1, width),
        soil,
        sun_tan.reshape(1, epochs),
        samples,
        occupancy,
    )
    return pl.pallas_call(
        conduct,
        out_shape=(
            jax.ShapeDtypeStruct(soil.shape, f32),
            jax.ShapeDtypeStruct((epochs, width), f32),
        ),
        in_specs=[vmem] * 4,
        out_specs=(vmem, vmem),
    )(*(pltpu.with_memory_space_constraint(value, pltpu.VMEM) for value in held))


def solution(mesh):
    in_specs = (
        P(None, ("basin", "recv", "src")),
        P(None, ("basin", "recv", "src")),
        P(("basin", "recv", "src")),
        P(("basin", "recv", "src")),
        P(("basin", "recv", "src")),
        P(None, ("basin", "recv", "src")),
        P(),
        P(("basin", "recv", "src"), None),
        P("basin", None),
    )
    out_specs = (P(None, ("basin", "recv", "src")), P(None, ("basin", "recv", "src")))
    return jax.shard_map(body, mesh=mesh, in_specs=in_specs, out_specs=out_specs, check_vma=False)
```

```python
import functools
import math

import jax
import jax.numpy as jnp
from jax import lax
from jax.experimental import pallas as pl
from jax.experimental.pallas import tpu as pltpu
from jax.sharding import PartitionSpec as P

solar_flux = 2.0
emissivity = 0.9
surface_gain = 0.1
shade_width = 0.1
reach_offset = 0.05
GROUP = 8
CHUNK = 16
TURNS = 128
PATCH = 64
PAIR = 4


def fourth(value):
    square = value * value
    return square * square


def column(row, count):
    wide = jnp.broadcast_to(row[:, :count], (count, count))
    here = lax.broadcasted_iota(jnp.int32, (count, count), 0) == lax.broadcasted_iota(
        jnp.int32, (count, count), 1
    )
    return jnp.sum(jnp.where(here, wide, 0.0), axis=1, keepdims=True)


def kernel(
    n_recv,
    n_src,
    pos_in,
    nrm_in,
    area_in,
    alb_in,
    cond_in,
    soil_in,
    tan_in,
    smp_in,
    occ_in,
    bounce_ref,
    heat_ref,
    cond_ref,
    soil_ref,
    pos_ref,
    nrm_ref,
    area_ref,
    alb_ref,
    tan_ref,
    smp_ref,
    occ_ref,
    near,
    far,
    planes,
    shifts,
    cols,
    view,
    direct_ref,
    lit_ref,
    tall_tan,
    radg,
    sems,
    loads,
):
    n = n_recv * n_src
    width = pos_ref.shape[1]
    n_samples = smp_ref.shape[1]
    epochs = tan_ref.shape[1]
    bits = width.bit_length() - 1
    few = n <= 16
    me = lax.axis_index("recv") * n_src + lax.axis_index("src")

    def peer(k):
        p = (me + (n - k)) & (n - 1)
        return {"recv": p >> (n_src.bit_length() - 1), "src": p & (n_src - 1)}

    def over(first, last, step):
        if few:
            for k in sorted(range(first, last), key=lambda k: abs(2 * k - n)):
                step(k)
        else:
            lax.fori_loop(first, last, lambda k, c: (step(k), c)[1], 0)

    barrier = pltpu.get_barrier_semaphore()
    over(
        1,
        n,
        lambda k: pl.semaphore_signal(
            barrier, inc=1, device_id=peer(k), device_id_type=pl.DeviceIdType.MESH
        ),
    )
    pairs = (
        (pos_in, pos_ref),
        (smp_in, smp_ref),
        (nrm_in, nrm_ref),
        (area_in, area_ref),
        (tan_in, tan_ref),
        (soil_in, soil_ref),
        (alb_in, alb_ref),
        (cond_in, cond_ref),
        (occ_in.at[pl.ds(me, 1)], occ_ref),
    )
    fetched = [
        pltpu.make_async_copy(there, here, loads.at[i]) for i, (there, here) in enumerate(pairs)
    ]
    for copy in fetched:
        copy.start()
    for copy in fetched[:4]:
        copy.wait()
    near[0, 0:3, :] = pos_ref[...]
    near[0, 3:4, 0:n_samples] = smp_ref[...].astype(jnp.float32)
    far[0, 0:3, :] = nrm_ref[...]
    far[0, 3:4, :] = area_ref[...]
    for copy in fetched[4:]:
        copy.wait()
    pl.semaphore_wait(barrier, n - 1)

    def send(ref, k, which):
        pltpu.make_async_remote_copy(
            src_ref=ref.at[0],
            dst_ref=ref.at[k],
            send_sem=sems.at[which],
            recv_sem=sems.at[which + 1],
            device_id=peer(k),
            device_id_type=pl.DeviceIdType.MESH,
        ).start()

    def everyone(ref, which):
        return pltpu.make_async_remote_copy(
            src_ref=ref.at[pl.ds(1, n - 1)],
            dst_ref=ref.at[pl.ds(1, n - 1)],
            send_sem=sems.at[which],
            recv_sem=sems.at[which + 1],
            device_id=peer(1),
            device_id_type=pl.DeviceIdType.MESH,
        )

    over(1, n, lambda k: send(near, k, 0))
    over(1, n, lambda k: send(far, k, 4))

    mine = near[0]
    tall = jnp.transpose(jnp.concatenate([mine, far[0]], axis=0))
    for c, at in enumerate((0, 1, 2, 4, 5, 6)):
        cols[c] = jnp.broadcast_to(tall[:, at : at + 1], (width, width))
    tan = column(tan_ref[...], epochs)
    angle = (
        2.0
        * math.pi
        * lax.broadcasted_iota(jnp.int32, (epochs, width), 0).astype(jnp.float32)
        / epochs
    )
    cos_e = 1.0 / jnp.sqrt(1.0 + tan * tan)
    incidence = (
        cos_e * jnp.cos(angle) * nrm_ref[0:1, :]
        + cos_e * jnp.sin(angle) * nrm_ref[1:2, :]
        + tan * cos_e * nrm_ref[2:3, :]
    )
    lit_ref[...] = solar_flux * jnp.maximum(incidence, 0.0)
    tall_tan[...] = jnp.broadcast_to(tan, (epochs, width))
    infrared = emissivity * fourth(soil_ref[0:1, :])

    everyone(near, 0).wait_recv()
    for c in range(3):
        planes[c] = near[:, c, :]
    rows = near[:, 3, :]
    shifts[0:n, :] = rows
    shifts[n : 2 * n, :] = rows

    lane = lax.broadcasted_iota(jnp.int32, (GROUP, width), 1)
    px, py, pz = (jnp.broadcast_to(mine[c : c + 1, :], (GROUP, width)) for c in range(3))

    def azimuths(group):
        offset = n - me + group * GROUP
        steps = shifts[pl.ds(offset, GROUP), :].astype(jnp.int32)
        best = jnp.full((GROUP, width), -1e30, jnp.float32)
        for s in range(n_samples):
            shift = jnp.broadcast_to(steps[:, s : s + 1], (GROUP, width))
            row = ((shift + (width - 1) - lane) >> bits) & (n - 1)
            within = row & (GROUP - 1)
            part = row >> (GROUP.bit_length() - 1)
            turn = (lane + shift) & (width - 1)
            found = []
            for c in range(3):
                picked = None
                for g in range(n // GROUP):
                    block = planes[c, g * GROUP : (g + 1) * GROUP, :]
                    got = jnp.take_along_axis(block, within, axis=0)
                    picked = got if picked is None else jnp.where(part == g, got, picked)
                found.append(jnp.take_along_axis(picked, turn, axis=1))
            dx = found[0] - px
            dy = found[1] - py
            reach = jnp.sqrt(dx * dx + dy * dy) + reach_offset
            best = jnp.maximum(best, (found[2] - pz) / reach)
        start = group * GROUP
        here = pl.ds(start if few else pl.multiple_of(start, GROUP), GROUP)
        direct = lit_ref[here, :] * jax.nn.sigmoid((tall_tan[here, :] - best) / shade_width)
        direct_ref[here, :] = direct
        radg[0, group] = (alb_ref[...] * direct + infrared).astype(jnp.bfloat16)
        over(1, n, lambda k: send(radg.at[:, group], k, 2))

    over(0, n // GROUP, azimuths)

    def see(k, carry):
        weight = occ_ref[0, lax.rem(me + k, n)].astype(jnp.float32)
        sx, sy, sz = (near[k, c : c + 1, :] for c in range(3))
        ox, oy, oz, size = (far[k, c : c + 1, :] for c in range(4))
        scale = size * weight / math.pi
        for i in range(width // CHUNK):
            at = slice(i * CHUNK, (i + 1) * CHUNK)
            dx = sx - cols[0, at, :]
            dy = sy - cols[1, at, :]
            dz = sz - cols[2, at, :]
            facing = cols[3, at, :] * dx + cols[4, at, :] * dy + cols[5, at, :] * dz
            toward = -(ox * dx + oy * dy + oz * dz)
            spread = dx * dx + dy * dy + dz * dz + size
            seen = jnp.maximum(facing, 0.0) * jnp.maximum(toward, 0.0) * scale
            view[k, at, :] = (seen / (spread * spread)).astype(jnp.bfloat16)
        return carry

    everyone(far, 4).wait_recv()
    lax.fori_loop(0, n, see, 0)
    everyone(radg, 2).wait_recv()

    def fold(k, total):
        sent = jnp.concatenate([radg[k, g] for g in range(epochs // GROUP)], axis=0)
        return total + lax.dot_general(
            sent, view[k], (((1,), (1,)), ((), ())), preferred_element_type=jnp.float32
        )

    total = jnp.zeros((epochs, width), jnp.float32)
    if few:
        for k in range(n):
            total = fold(k, total)
    else:
        total = lax.fori_loop(0, n, fold, total)
    bounce_ref[...] = total
    keep = surface_gain * (1.0 - alb_ref[...])
    heat_ref[...] = keep * (direct_ref[...] + total)
    everyone(near, 0).wait_send()
    everyone(far, 4).wait_send()
    everyone(radg, 2).wait_send()


def step(
    n_recv,
    n_src,
    pos_in,
    nrm_in,
    area_in,
    alb_in,
    cond_in,
    soil_in,
    tan_in,
    smp_in,
    occ_in,
    bounce_ref,
    heat_ref,
    cond_ref,
    soil_ref,
    tan_ref,
    occ_ref,
    facts,
    offsets,
    smp,
    planes,
    table,
    cols,
    view,
    sun_ref,
    direct_ref,
    lit_ref,
    hello,
    sent,
    got,
    loads,
):
    n = n_recv * n_src
    width = soil_ref.shape[1]
    n_samples = smp.shape[2]
    epochs = tan_ref.shape[1]
    bits = width.bit_length() - 1
    n_facts = facts.shape[0]
    chip_bits = n_src.bit_length() - 1
    quarter = n // 4
    pitch = 2 * n + 8
    me = lax.axis_index("recv") * n_src + lax.axis_index("src")
    chip = lax.axis_index("recv")

    def device(p):
        return {"recv": p >> chip_bits, "src": p & (n_src - 1)}

    def greet(sem, p):
        pl.semaphore_signal(sem, inc=1, device_id=device(p), device_id_type=pl.DeviceIdType.MESH)

    def each(first, last, do):
        lax.fori_loop(first, last, lambda p, c: (do(p), c)[1], 0)

    own = pl.ds(me, 1)
    fill = [(pos_in.at[pl.ds(c, 1)], facts.at[c, own]) for c in range(3)]
    fill += [(nrm_in.at[pl.ds(c, 1)], facts.at[3 + c, own]) for c in range(3)]
    fill += [(area_in, facts.at[6, own]), (alb_in, facts.at[7, own])]
    fill += [(soil_in.at[pl.ds(0, 1)], facts.at[8, own])]
    for there, here in fill:
        pltpu.make_async_copy(there, here, loads.at[0]).start()
    pairs = (
        (smp_in, offsets.at[me]),
        (tan_in, tan_ref),
        (soil_in, soil_ref),
        (cond_in, cond_ref),
        (occ_in.at[own], occ_ref),
    )
    fetched = [
        pltpu.make_async_copy(there, here, loads.at[1 + i]) for i, (there, here) in enumerate(pairs)
    ]
    for copy in fetched:
        copy.start()
    barrier = pltpu.get_barrier_semaphore()
    each(me + 1, n, lambda p: greet(barrier, p))
    pl.when(me > 0)(lambda: pl.semaphore_wait(barrier, me))
    each(0, me, lambda p: greet(hello.at[chip], p))

    def remote(slots, to, sem):
        return pltpu.make_async_remote_copy(
            src_ref=facts.at[:, slots],
            dst_ref=facts.at[:, slots],
            send_sem=sent.at[0],
            recv_sem=got.at[sem],
            device_id=device(to),
            device_id_type=pl.DeviceIdType.MESH,
        )

    def remote_offsets(slot, to):
        return pltpu.make_async_remote_copy(
            src_ref=offsets.at[slot],
            dst_ref=offsets.at[slot],
            send_sem=sent.at[1],
            recv_sem=got.at[n_recv + slot // quarter],
            device_id=device(to),
            device_id_type=pl.DeviceIdType.MESH,
        )

    def tell(p):
        remote(own, p, chip).start()
        remote_offsets(me, p).start()

    pltpu.make_async_copy(facts.at[:, own], facts.at[:, own], loads.at[0]).wait()
    fetched[0].wait()
    each(0, me, tell)
    for copy in fetched[1:]:
        copy.wait()

    mine = jnp.concatenate([facts[0:6, me, :], facts[0:2, me, :]], axis=0)
    tall = jnp.transpose(mine)
    for c in range(6):
        cols[c] = jnp.broadcast_to(tall[:, c : c + 1], (width, width))
    tan = column(tan_ref[...], epochs)
    angle = (
        2.0
        * math.pi
        * lax.broadcasted_iota(jnp.int32, (epochs, width), 0).astype(jnp.float32)
        / epochs
    )
    cos_e = 1.0 / jnp.sqrt(1.0 + tan * tan)
    sun_ref[0] = cos_e * jnp.cos(angle)
    sun_ref[1] = cos_e * jnp.sin(angle)
    sun_ref[2] = jnp.broadcast_to(tan * cos_e, (epochs, width))
    sun_ref[3] = jnp.broadcast_to(tan, (epochs, width))

    def glimpses(p):
        weight = occ_ref[0, p].astype(jnp.float32)
        row = pl.ds(p, 1)
        sx, sy, sz, ox, oy, oz, size = (facts[c, row, :] for c in range(7))
        scale = size * weight / math.pi

        def glimpse(i):
            at = slice(i * CHUNK, (i + 1) * CHUNK)
            dx = sx - cols[0, at, :]
            dy = sy - cols[1, at, :]
            dz = sz - cols[2, at, :]
            facing = cols[3, at, :] * dx + cols[4, at, :] * dy + cols[5, at, :] * dz
            toward = -(ox * dx + oy * dy + oz * dz)
            spread = dx * dx + dy * dy + dz * dz + size
            seen = jnp.maximum(facing, 0.0) * jnp.maximum(toward, 0.0) * scale
            view[p, at, :] = (seen / (spread * spread)).astype(jnp.bfloat16)

        return [functools.partial(glimpse, i) for i in range(width // CHUNK)]

    def see(p):
        for glimpse in glimpses(p):
            glimpse()

    see(me)
    for other in range(1, n_src):
        p = me ^ other

        def answer_here():
            pl.semaphore_wait(hello.at[chip], 1)
            tell(p)

        pl.when(p > me)(answer_here)

    def answer(g):
        pl.semaphore_wait(hello.at[g], n_src)
        for core in range(n_src):
            tell(g * n_src + core)

    each(chip + 1, n_recv, answer)

    for other in range(1, n_src):
        remote(pl.ds(me ^ other, 1), me ^ other, chip).wait_recv()
        see(me ^ other)

    def arrive(m):
        g = chip ^ m
        remote(pl.ds(g * n_src, n_src), me ^ 1, g).wait_recv()

    def arrive_and_see(m):
        arrive(m)
        for core in range(n_src):
            see((chip ^ m) * n_src + core)

    late = n_recv - n_recv // 4
    each(1, late, arrive_and_see)

    def spread_rows():
        planes[0:24, :] = planes[3 * n : 3 * n + 24, :]
        planes[3 * n + 24 : 3 * n + 48, :] = planes[24:48, :]

    def place(m):
        start = ((me // quarter) ^ m) * quarter
        for c in range(3):
            put = pl.ds((8 + start) * 3 + c, quarter, stride=3)
            planes[put, :] = facts[c, pl.ds(start, quarter), :]

    for m in range(3):
        place(m)
    gap = ((me // quarter) ^ 3) * quarter
    planes[pl.ds((8 + gap) * 3, 3 * quarter), :] = jnp.zeros((3 * quarter, width), jnp.float32)
    spread_rows()
    lane = lax.broadcasted_iota(jnp.int32, (8, width), 1)

    def turn(r, here, after):
        mixed = jnp.where(lane >= r, here, after)
        return pltpu.roll(mixed, (width - r) & (width - 1), 1)

    def spin(i, carry):
        for j in range(TURNS):
            r = i * TURNS + j
            for g in range(3 * n // 8):
                at = 24 + g * 8
                turned = turn(r, planes[at : at + 8, :], planes[at + 3 : at + 11, :])
                table[pl.ds(r * (3 * pitch) + at, 8), :] = turned
                table[pl.ds(r * (3 * pitch) + at + 3 * n, 8), :] = turned
        return carry

    def samples_of(m, count):
        slots = pl.ds(0, count)
        return pltpu.make_async_remote_copy(
            src_ref=offsets.at[slots],
            dst_ref=offsets.at[slots],
            send_sem=sent.at[1],
            recv_sem=got.at[n_recv + ((me // quarter) ^ m)],
            device_id=device(me ^ 1),
            device_id_type=pl.DeviceIdType.MESH,
        )

    def to_scalars(m):
        slots = pl.ds(((me // quarter) ^ m) * quarter, quarter)
        return pltpu.make_async_copy(offsets.at[slots], smp.at[slots], loads.at[6 + m])

    for m in range(3):
        samples_of(m, quarter - (m == 0)).wait_recv()
        to_scalars(m).start()
    lax.fori_loop(0, width // TURNS, spin, 0)
    each(late, n_recv, arrive)
    samples_of(3, quarter).wait_recv()
    to_scalars(3).start()
    place(3)
    spread_rows()

    at = (7 + gap) * 3
    halves = [8 * k for k in range(2)]
    window = [[planes[pl.ds(at + k + half, 8), :] for k in (0, 3)] for half in halves]

    def respin(i, carry):
        blocks = quarter * PATCH // width
        todo = [g for j in range(blocks) for g in glimpses(gap + i * blocks + j)]
        for j in range(PATCH):
            r = i * PATCH + j
            for half, (here, after) in zip(halves, window):
                turned = turn(r, here, after)
                table[pl.ds(r * (3 * pitch) + at + half, 8), :] = turned
                table[pl.ds(r * (3 * pitch) + at + half + 3 * n, 8), :] = turned
            if j % (PATCH // len(todo)) == 0:
                todo[j // (PATCH // len(todo))]()
        return carry

    lax.fori_loop(0, width // PATCH, respin, 0)
    for m in range(3):
        to_scalars(m).wait()

    def horizon(a):
        here = [[facts[c, g * 8 : g * 8 + 8, :] for g in range(n // 8)] for c in range(3)]
        best = [jnp.full((8, width), -1e30, jnp.float32) for g in range(n // 8)]
        for s in range(n_samples):
            shift = smp[a, 0, s]
            start = ((shift & (width - 1)) * pitch + (shift >> bits) + 8) * 3
            for g in range(n // 8):
                fx, fy, fz = (
                    table[pl.ds(start + g * 24 + c, 8, stride=3), :] for c in range(3)
                )
                dx = fx - here[0][g]
                dy = fy - here[1][g]
                reach = 1.0 / lax.rsqrt(dx * dx + dy * dy) + reach_offset
                best[g] = jnp.maximum(best[g], (fz - here[2][g]) / reach)
        line = pl.ds(a, 1)
        cx, cy, cz, tans = (sun_ref[c, line, :] for c in range(4))
        for g in range(n // 8):
            at = slice(g * 8, g * 8 + 8)
            incidence = cx * facts[3, at, :] + cy * facts[4, at, :] + cz * facts[5, at, :]
            shade = jax.nn.sigmoid((tans - best[g]) / shade_width)
            direct = solar_flux * jnp.maximum(incidence, 0.0) * shade
            put = pl.ds(pl.multiple_of(a * n + g * 8, 8), 8)
            direct_ref[put, :] = direct
            lit_ref[put, :] = facts[7, at, :] * direct + emissivity * fourth(facts[8, at, :])

    shared = epochs // 4
    core = me & 1
    partner = me ^ 1

    def azimuth(order):
        return ((me // quarter) ^ (order // quarter)) * quarter + (order & (quarter - 1))

    def swap(ref, which):
        return pltpu.make_async_remote_copy(
            src_ref=ref,
            dst_ref=ref,
            send_sem=sent.at[2 + which],
            recv_sem=got.at[n_recv + 4 + which],
            device_id=device(partner),
            device_id_type=pl.DeviceIdType.MESH,
        )

    def swaps(first, facet):
        start = pl.multiple_of(azimuth(first) * n, 8)
        lines = [direct_ref.at[pl.ds(start + k * n + facet, 1)] for k in range(shared)]
        return [swap(lit_ref.at[pl.ds(start, shared * n)], 0)] + [swap(line, 1) for line in lines]

    swapped = (swap(lit_ref.at[pl.ds(0, shared * n)], 0), swap(direct_ref.at[pl.ds(0, shared)], 1))

    def horizons(i, carry):
        @pl.when(i == shared // PAIR)
        def _():
            for copy in swaps(core * shared, partner):
                copy.start()

        @pl.when(i == 2 * shared // PAIR)
        def _():
            to_scalars(3).wait()

        first = jnp.where(i < shared // PAIR, core * shared, shared) + i * PAIR
        for j in range(PAIR):
            horizon(azimuth(first + j))
        return carry

    lax.fori_loop(0, 3 * shared // PAIR, horizons, 0)
    for copy in swapped:
        copy.wait_recv()

    total = jnp.zeros((epochs, width), jnp.float32)
    for p in range(n):
        total = total + lax.dot_general(
            lit_ref[pl.ds(p, epochs, stride=n), :].astype(jnp.bfloat16),
            view[p],
            (((1,), (1,)), ((), ())),
            preferred_element_type=jnp.float32,
        )
    bounce_ref[...] = total
    keep = surface_gain * (1.0 - facts[7, own, :])
    heat_ref[...] = keep * (direct_ref[pl.ds(me, epochs, stride=n), :] + total)
    remote(pl.ds(0, n - 1), me ^ 1, 0).wait_send()
    samples_of(0, n - 1).wait_send()
    for copy in swapped:
        copy.wait_send()


def conduct(bounce_in, heat_ref, cond_ref, soil_ref, final_ref, bounce_ref):
    layers, width = soil_ref.shape
    epochs = heat_ref.shape[0]
    bounce_ref[...] = bounce_in[...]
    cond = cond_ref[...]
    first = lax.broadcasted_iota(jnp.int32, (layers, width), 0) == 0
    last = lax.broadcasted_iota(jnp.int32, (layers, width), 0) == layers - 1

    def advance(t, temps):
        below = jnp.where(last, temps, pltpu.roll(temps, layers - 1, 0))
        above = jnp.where(first, temps, pltpu.roll(temps, 1, 0))
        temps = temps + cond * ((below - temps) - (temps - above))
        gain = heat_ref[pl.ds(t, 1), :] - (surface_gain * emissivity) * fourth(temps)
        return jnp.where(first, temps + gain, temps)

    temps = soil_ref[...]
    if epochs <= 16:
        for t in range(epochs):
            temps = advance(t, temps)
    else:
        temps = lax.fori_loop(0, epochs, advance, temps)
    final_ref[...] = temps


def body(positions, normals, area, albedo, conductivity, soil, sun_tan, samples, occupancy):
    n_recv = lax.axis_size("recv")
    n_src = lax.axis_size("src")
    n = n_recv * n_src
    width = positions.shape[1]
    epochs = sun_tan.shape[0]
    vmem = pl.BlockSpec(memory_space=pltpu.VMEM)
    f32 = jnp.float32
    n_samples = samples.shape[1]
    if n <= 16:
        program = step
        scratch = [
            pltpu.VMEM((1, epochs), f32),
            pltpu.SMEM((1, occupancy.shape[1]), jnp.int32),
            pltpu.VMEM((9, n, width), f32),
            pltpu.VMEM((n, 1, n_samples), jnp.int32),
            pltpu.SMEM((n, 1, n_samples), jnp.int32),
            pltpu.VMEM((3 * (n + 16), width), f32),
            pltpu.VMEM((3 * width * (2 * n + 8) + 8, width), f32),
            pltpu.VMEM((6, width, width), f32),
            pltpu.VMEM((n, width, width), jnp.bfloat16),
            pltpu.VMEM((4, epochs, width), f32),
            pltpu.VMEM((epochs * n, width), f32),
            pltpu.VMEM((epochs * n, width), f32),
            pltpu.SemaphoreType.REGULAR((n_recv,)),
            pltpu.SemaphoreType.DMA((4,)),
            pltpu.SemaphoreType.DMA((n_recv + 6,)),
            pltpu.SemaphoreType.DMA((10,)),
        ]
    else:
        program = kernel
        scratch = [
            pltpu.VMEM((3, width), f32),
            pltpu.VMEM((3, width), f32),
            pltpu.VMEM((1, width), f32),
            pltpu.VMEM((1, width), f32),
            pltpu.VMEM((1, epochs), f32),
            pltpu.VMEM((1, n_samples), jnp.int32),
            pltpu.SMEM((1, occupancy.shape[1]), jnp.int32),
            pltpu.VMEM((n, 4, width), f32),
            pltpu.VMEM((n, 4, width), f32),
            pltpu.VMEM((3, n, width), f32),
            pltpu.VMEM((2 * n, width), f32),
            pltpu.VMEM((6, width, width), f32),
            pltpu.VMEM((n, width, width), jnp.bfloat16),
            pltpu.VMEM((epochs, width), f32),
            pltpu.VMEM((epochs, width), f32),
            pltpu.VMEM((epochs, width), f32),
            pltpu.VMEM((n, epochs // GROUP, GROUP, width), jnp.bfloat16),
            pltpu.SemaphoreType.DMA((6,)),
            pltpu.SemaphoreType.DMA((9,)),
        ]
    held = pl.pallas_call(
        functools.partial(program, n_recv, n_src),
        out_shape=(
            pltpu.VMEM((epochs, width), f32),
            pltpu.VMEM((epochs, width), f32),
            pltpu.VMEM((1, width), f32),
            pltpu.VMEM(soil.shape, f32),
        ),
        in_specs=[pl.BlockSpec(memory_space=pl.ANY)] * 9,
        out_specs=(vmem,) * 4,
        scratch_shapes=scratch,
        compiler_params=pltpu.CompilerParams(collective_id=0, has_side_effects=True),
    )(
        positions,
        normals,
        area.reshape(1, width),
        albedo.reshape(1, width),
        conductivity.reshape(1, width),
        soil,
        sun_tan.reshape(1, epochs),
        samples,
        occupancy,
    )
    return pl.pallas_call(
        conduct,
        out_shape=(
            jax.ShapeDtypeStruct(soil.shape, f32),
            jax.ShapeDtypeStruct((epochs, width), f32),
        ),
        in_specs=[vmem] * 4,
        out_specs=(vmem, vmem),
    )(*(pltpu.with_memory_space_constraint(value, pltpu.VMEM) for value in held))


def solution(mesh):
    in_specs = (
        P(None, ("basin", "recv", "src")),
        P(None, ("basin", "recv", "src")),
        P(("basin", "recv", "src")),
        P(("basin", "recv", "src")),
        P(("basin", "recv", "src")),
        P(None, ("basin", "recv", "src")),
        P(),
        P(("basin", "recv", "src"), None),
        P("basin", None),
    )
    out_specs = (P(None, ("basin", "recv", "src")), P(None, ("basin", "recv", "src")))
    return jax.shard_map(body, mesh=mesh, in_specs=in_specs, out_specs=out_specs, check_vma=False)
```

```python
import functools
import math

import jax
import jax.numpy as jnp
from jax import lax
from jax.experimental import pallas as pl
from jax.experimental.pallas import tpu as pltpu
from jax.sharding import PartitionSpec as P

solar_flux = 2.0
emissivity = 0.9
surface_gain = 0.1
shade_width = 0.1
reach_offset = 0.05
GROUP = 8
CHUNK = 16
TURNS = 128
PATCH = 64
PAIR = 4


def fourth(value):
    square = value * value
    return square * square


def column(row, count):
    wide = jnp.broadcast_to(row[:, :count], (count, count))
    here = lax.broadcasted_iota(jnp.int32, (count, count), 0) == lax.broadcasted_iota(
        jnp.int32, (count, count), 1
    )
    return jnp.sum(jnp.where(here, wide, 0.0), axis=1, keepdims=True)


def kernel(
    n_recv,
    n_src,
    pos_in,
    nrm_in,
    area_in,
    alb_in,
    cond_in,
    soil_in,
    tan_in,
    smp_in,
    occ_in,
    bounce_ref,
    heat_ref,
    cond_ref,
    soil_ref,
    pos_ref,
    nrm_ref,
    area_ref,
    alb_ref,
    tan_ref,
    smp_ref,
    occ_ref,
    near,
    far,
    planes,
    shifts,
    cols,
    view,
    direct_ref,
    lit_ref,
    tall_tan,
    radg,
    sems,
    loads,
):
    n = n_recv * n_src
    width = pos_ref.shape[1]
    n_samples = smp_ref.shape[1]
    epochs = tan_ref.shape[1]
    bits = width.bit_length() - 1
    few = n <= 16
    me = lax.axis_index("recv") * n_src + lax.axis_index("src")

    def peer(k):
        p = (me + (n - k)) & (n - 1)
        return {"recv": p >> (n_src.bit_length() - 1), "src": p & (n_src - 1)}

    def over(first, last, step):
        if few:
            for k in sorted(range(first, last), key=lambda k: abs(2 * k - n)):
                step(k)
        else:
            lax.fori_loop(first, last, lambda k, c: (step(k), c)[1], 0)

    barrier = pltpu.get_barrier_semaphore()
    over(
        1,
        n,
        lambda k: pl.semaphore_signal(
            barrier, inc=1, device_id=peer(k), device_id_type=pl.DeviceIdType.MESH
        ),
    )
    pairs = (
        (pos_in, pos_ref),
        (smp_in, smp_ref),
        (nrm_in, nrm_ref),
        (area_in, area_ref),
        (tan_in, tan_ref),
        (soil_in, soil_ref),
        (alb_in, alb_ref),
        (cond_in, cond_ref),
        (occ_in.at[pl.ds(me, 1)], occ_ref),
    )
    fetched = [
        pltpu.make_async_copy(there, here, loads.at[i]) for i, (there, here) in enumerate(pairs)
    ]
    for copy in fetched:
        copy.start()
    for copy in fetched[:4]:
        copy.wait()
    near[0, 0:3, :] = pos_ref[...]
    near[0, 3:4, 0:n_samples] = smp_ref[...].astype(jnp.float32)
    far[0, 0:3, :] = nrm_ref[...]
    far[0, 3:4, :] = area_ref[...]
    for copy in fetched[4:]:
        copy.wait()
    pl.semaphore_wait(barrier, n - 1)

    def send(ref, k, which):
        pltpu.make_async_remote_copy(
            src_ref=ref.at[0],
            dst_ref=ref.at[k],
            send_sem=sems.at[which],
            recv_sem=sems.at[which + 1],
            device_id=peer(k),
            device_id_type=pl.DeviceIdType.MESH,
        ).start()

    def everyone(ref, which):
        return pltpu.make_async_remote_copy(
            src_ref=ref.at[pl.ds(1, n - 1)],
            dst_ref=ref.at[pl.ds(1, n - 1)],
            send_sem=sems.at[which],
            recv_sem=sems.at[which + 1],
            device_id=peer(1),
            device_id_type=pl.DeviceIdType.MESH,
        )

    over(1, n, lambda k: send(near, k, 0))
    over(1, n, lambda k: send(far, k, 4))

    mine = near[0]
    tall = jnp.transpose(jnp.concatenate([mine, far[0]], axis=0))
    for c, at in enumerate((0, 1, 2, 4, 5, 6)):
        cols[c] = jnp.broadcast_to(tall[:, at : at + 1], (width, width))
    tan = column(tan_ref[...], epochs)
    angle = (
        2.0
        * math.pi
        * lax.broadcasted_iota(jnp.int32, (epochs, width), 0).astype(jnp.float32)
        / epochs
    )
    cos_e = 1.0 / jnp.sqrt(1.0 + tan * tan)
    incidence = (
        cos_e * jnp.cos(angle) * nrm_ref[0:1, :]
        + cos_e * jnp.sin(angle) * nrm_ref[1:2, :]
        + tan * cos_e * nrm_ref[2:3, :]
    )
    lit_ref[...] = solar_flux * jnp.maximum(incidence, 0.0)
    tall_tan[...] = jnp.broadcast_to(tan, (epochs, width))
    infrared = emissivity * fourth(soil_ref[0:1, :])

    everyone(near, 0).wait_recv()
    for c in range(3):
        planes[c] = near[:, c, :]
    rows = near[:, 3, :]
    shifts[0:n, :] = rows
    shifts[n : 2 * n, :] = rows

    lane = lax.broadcasted_iota(jnp.int32, (GROUP, width), 1)
    px, py, pz = (jnp.broadcast_to(mine[c : c + 1, :], (GROUP, width)) for c in range(3))

    def azimuths(group):
        offset = n - me + group * GROUP
        steps = shifts[pl.ds(offset, GROUP), :].astype(jnp.int32)
        best = jnp.full((GROUP, width), -1e30, jnp.float32)
        for s in range(n_samples):
            shift = jnp.broadcast_to(steps[:, s : s + 1], (GROUP, width))
            row = ((shift + (width - 1) - lane) >> bits) & (n - 1)
            within = row & (GROUP - 1)
            part = row >> (GROUP.bit_length() - 1)
            turn = (lane + shift) & (width - 1)
            found = []
            for c in range(3):
                picked = None
                for g in range(n // GROUP):
                    block = planes[c, g * GROUP : (g + 1) * GROUP, :]
                    got = jnp.take_along_axis(block, within, axis=0)
                    picked = got if picked is None else jnp.where(part == g, got, picked)
                found.append(jnp.take_along_axis(picked, turn, axis=1))
            dx = found[0] - px
            dy = found[1] - py
            reach = jnp.sqrt(dx * dx + dy * dy) + reach_offset
            best = jnp.maximum(best, (found[2] - pz) / reach)
        start = group * GROUP
        here = pl.ds(start if few else pl.multiple_of(start, GROUP), GROUP)
        direct = lit_ref[here, :] * jax.nn.sigmoid((tall_tan[here, :] - best) / shade_width)
        direct_ref[here, :] = direct
        radg[0, group] = (alb_ref[...] * direct + infrared).astype(jnp.bfloat16)
        over(1, n, lambda k: send(radg.at[:, group], k, 2))

    over(0, n // GROUP, azimuths)

    def see(k, carry):
        weight = occ_ref[0, lax.rem(me + k, n)].astype(jnp.float32)
        sx, sy, sz = (near[k, c : c + 1, :] for c in range(3))
        ox, oy, oz, size = (far[k, c : c + 1, :] for c in range(4))
        scale = size * weight / math.pi
        for i in range(width // CHUNK):
            at = slice(i * CHUNK, (i + 1) * CHUNK)
            dx = sx - cols[0, at, :]
            dy = sy - cols[1, at, :]
            dz = sz - cols[2, at, :]
            facing = cols[3, at, :] * dx + cols[4, at, :] * dy + cols[5, at, :] * dz
            toward = -(ox * dx + oy * dy + oz * dz)
            spread = dx * dx + dy * dy + dz * dz + size
            seen = jnp.maximum(facing, 0.0) * jnp.maximum(toward, 0.0) * scale
            view[k, at, :] = (seen / (spread * spread)).astype(jnp.bfloat16)
        return carry

    everyone(far, 4).wait_recv()
    lax.fori_loop(0, n, see, 0)
    everyone(radg, 2).wait_recv()

    def fold(k, total):
        sent = jnp.concatenate([radg[k, g] for g in range(epochs // GROUP)], axis=0)
        return total + lax.dot_general(
            sent, view[k], (((1,), (1,)), ((), ())), preferred_element_type=jnp.float32
        )

    total = jnp.zeros((epochs, width), jnp.float32)
    if few:
        for k in range(n):
            total = fold(k, total)
    else:
        total = lax.fori_loop(0, n, fold, total)
    bounce_ref[...] = total
    keep = surface_gain * (1.0 - alb_ref[...])
    heat_ref[...] = keep * (direct_ref[...] + total)
    everyone(near, 0).wait_send()
    everyone(far, 4).wait_send()
    everyone(radg, 2).wait_send()


def step(
    n_recv,
    n_src,
    pos_in,
    nrm_in,
    area_in,
    alb_in,
    cond_in,
    soil_in,
    tan_in,
    smp_in,
    occ_in,
    bounce_ref,
    heat_ref,
    cond_ref,
    soil_ref,
    tan_ref,
    occ_ref,
    facts,
    offsets,
    smp,
    planes,
    table,
    cols,
    view,
    sun_ref,
    direct_ref,
    lit_ref,
    hello,
    sent,
    got,
    loads,
):
    n = n_recv * n_src
    width = soil_ref.shape[1]
    n_samples = smp.shape[2]
    epochs = tan_ref.shape[1]
    bits = width.bit_length() - 1
    n_facts = facts.shape[0]
    chip_bits = n_src.bit_length() - 1
    quarter = n // 4
    pitch = 2 * n + 8
    me = lax.axis_index("recv") * n_src + lax.axis_index("src")
    chip = lax.axis_index("recv")

    def device(p):
        return {"recv": p >> chip_bits, "src": p & (n_src - 1)}

    def greet(sem, p):
        pl.semaphore_signal(sem, inc=1, device_id=device(p), device_id_type=pl.DeviceIdType.MESH)

    def each(first, last, do):
        lax.fori_loop(first, last, lambda p, c: (do(p), c)[1], 0)

    own = pl.ds(me, 1)
    fill = [(pos_in.at[pl.ds(c, 1)], facts.at[c, own]) for c in range(3)]
    fill += [(nrm_in.at[pl.ds(c, 1)], facts.at[3 + c, own]) for c in range(3)]
    fill += [(area_in, facts.at[6, own]), (alb_in, facts.at[7, own])]
    fill += [(soil_in.at[pl.ds(0, 1)], facts.at[8, own])]
    for there, here in fill:
        pltpu.make_async_copy(there, here, loads.at[0]).start()
    pairs = (
        (smp_in, offsets.at[me]),
        (tan_in, tan_ref),
        (soil_in, soil_ref),
        (cond_in, cond_ref),
        (occ_in.at[own], occ_ref),
    )
    fetched = [
        pltpu.make_async_copy(there, here, loads.at[1 + i]) for i, (there, here) in enumerate(pairs)
    ]
    for copy in fetched:
        copy.start()
    barrier = pltpu.get_barrier_semaphore()
    each(me + 1, n, lambda p: greet(barrier, p))
    pl.when(me > 0)(lambda: pl.semaphore_wait(barrier, me))
    each(0, me, lambda p: greet(hello.at[chip], p))

    def remote(slots, to, sem):
        return pltpu.make_async_remote_copy(
            src_ref=facts.at[:, slots],
            dst_ref=facts.at[:, slots],
            send_sem=sent.at[0],
            recv_sem=got.at[sem],
            device_id=device(to),
            device_id_type=pl.DeviceIdType.MESH,
        )

    def remote_offsets(slot, to):
        return pltpu.make_async_remote_copy(
            src_ref=offsets.at[slot],
            dst_ref=offsets.at[slot],
            send_sem=sent.at[1],
            recv_sem=got.at[n_recv + slot // quarter],
            device_id=device(to),
            device_id_type=pl.DeviceIdType.MESH,
        )

    def tell(p):
        remote(own, p, chip).start()
        remote_offsets(me, p).start()

    pltpu.make_async_copy(facts.at[:, own], facts.at[:, own], loads.at[0]).wait()
    fetched[0].wait()
    each(0, me, tell)
    for copy in fetched[1:]:
        copy.wait()

    mine = jnp.concatenate([facts[0:6, me, :], facts[0:2, me, :]], axis=0)
    tall = jnp.transpose(mine)
    for c in range(6):
        cols[c] = jnp.broadcast_to(tall[:, c : c + 1], (width, width))
    tan = column(tan_ref[...], epochs)
    angle = (
        2.0
        * math.pi
        * lax.broadcasted_iota(jnp.int32, (epochs, width), 0).astype(jnp.float32)
        / epochs
    )
    cos_e = 1.0 / jnp.sqrt(1.0 + tan * tan)
    sun_ref[0] = cos_e * jnp.cos(angle)
    sun_ref[1] = cos_e * jnp.sin(angle)
    sun_ref[2] = jnp.broadcast_to(tan * cos_e, (epochs, width))
    sun_ref[3] = jnp.broadcast_to(tan, (epochs, width))

    def glimpses(p):
        weight = occ_ref[0, p].astype(jnp.float32)
        row = pl.ds(p, 1)
        sx, sy, sz, ox, oy, oz, size = (facts[c, row, :] for c in range(7))
        scale = size * weight / math.pi

        def glimpse(i):
            at = slice(i * CHUNK, (i + 1) * CHUNK)
            dx = sx - cols[0, at, :]
            dy = sy - cols[1, at, :]
            dz = sz - cols[2, at, :]
            facing = cols[3, at, :] * dx + cols[4, at, :] * dy + cols[5, at, :] * dz
            toward = -(ox * dx + oy * dy + oz * dz)
            spread = dx * dx + dy * dy + dz * dz + size
            seen = jnp.maximum(facing, 0.0) * jnp.maximum(toward, 0.0) * scale
            view[p, at, :] = (seen / (spread * spread)).astype(jnp.bfloat16)

        return [functools.partial(glimpse, i) for i in range(width // CHUNK)]

    def see(p):
        for glimpse in glimpses(p):
            glimpse()

    see(me)
    for other in range(1, n_src):
        p = me ^ other

        def answer_here():
            pl.semaphore_wait(hello.at[chip], 1)
            tell(p)

        pl.when(p > me)(answer_here)

    def answer(g):
        pl.semaphore_wait(hello.at[g], n_src)
        for core in range(n_src):
            tell(g * n_src + core)

    each(chip + 1, n_recv, answer)

    for other in range(1, n_src):
        remote(pl.ds(me ^ other, 1), me ^ other, chip).wait_recv()
        see(me ^ other)

    def arrive(m):
        g = chip ^ m
        remote(pl.ds(g * n_src, n_src), me ^ 1, g).wait_recv()

    def arrive_and_see(m):
        arrive(m)
        for core in range(n_src):
            see((chip ^ m) * n_src + core)

    late = n_recv - n_recv // 4
    each(1, late, arrive_and_see)

    def spread_rows():
        planes[0:24, :] = planes[3 * n : 3 * n + 24, :]
        planes[3 * n + 24 : 3 * n + 48, :] = planes[24:48, :]

    def place(m):
        start = ((me // quarter) ^ m) * quarter
        for c in range(3):
            put = pl.ds((8 + start) * 3 + c, quarter, stride=3)
            planes[put, :] = facts[c, pl.ds(start, quarter), :]

    for m in range(3):
        place(m)
    gap = ((me // quarter) ^ 3) * quarter
    planes[pl.ds((8 + gap) * 3, 3 * quarter), :] = jnp.zeros((3 * quarter, width), jnp.float32)
    spread_rows()
    lane = lax.broadcasted_iota(jnp.int32, (8, width), 1)

    def turn(r, here, after):
        mixed = jnp.where(lane >= r, here, after)
        return pltpu.roll(mixed, (width - r) & (width - 1), 1)

    def spin(i, carry):
        for j in range(TURNS):
            r = i * TURNS + j
            for g in range(3 * n // 8):
                at = 24 + g * 8
                turned = turn(r, planes[at : at + 8, :], planes[at + 3 : at + 11, :])
                table[pl.ds(r * (3 * pitch) + at, 8), :] = turned
                table[pl.ds(r * (3 * pitch) + at + 3 * n, 8), :] = turned
        return carry

    def samples_of(m, count):
        slots = pl.ds(0, count)
        return pltpu.make_async_remote_copy(
            src_ref=offsets.at[slots],
            dst_ref=offsets.at[slots],
            send_sem=sent.at[1],
            recv_sem=got.at[n_recv + ((me // quarter) ^ m)],
            device_id=device(me ^ 1),
            device_id_type=pl.DeviceIdType.MESH,
        )

    def to_scalars(m):
        slots = pl.ds(((me // quarter) ^ m) * quarter, quarter)
        return pltpu.make_async_copy(offsets.at[slots], smp.at[slots], loads.at[6 + m // 3])

    for m in range(3):
        samples_of(m, quarter - (m == 0)).wait_recv()
        to_scalars(m).start()
    lax.fori_loop(0, width // TURNS, spin, 0)
    each(late, n_recv, arrive)
    samples_of(3, quarter).wait_recv()
    to_scalars(3).start()
    place(3)
    spread_rows()

    at = (7 + gap) * 3
    halves = [8 * k for k in range(2)]
    window = [[planes[pl.ds(at + k + half, 8), :] for k in (0, 3)] for half in halves]

    def respin(i, carry):
        blocks = quarter * PATCH // width
        todo = [g for j in range(blocks) for g in glimpses(gap + i * blocks + j)]
        for j in range(PATCH):
            r = i * PATCH + j
            for half, (here, after) in zip(halves, window):
                turned = turn(r, here, after)
                table[pl.ds(r * (3 * pitch) + at + half, 8), :] = turned
                table[pl.ds(r * (3 * pitch) + at + half + 3 * n, 8), :] = turned
            if j % (PATCH // len(todo)) == 0:
                todo[j // (PATCH // len(todo))]()
        return carry

    lax.fori_loop(0, width // PATCH, respin, 0)
    early_rows = pl.ds(0, 3 * quarter)
    pltpu.make_async_copy(offsets.at[early_rows], smp.at[early_rows], loads.at[6]).wait()

    def horizon(a):
        here = [[facts[c, g * 8 : g * 8 + 8, :] for g in range(n // 8)] for c in range(3)]
        best = [jnp.full((8, width), -1e30, jnp.float32) for g in range(n // 8)]
        for s in range(n_samples):
            shift = smp[a, 0, s]
            start = ((shift & (width - 1)) * pitch + (shift >> bits) + 8) * 3
            for g in range(n // 8):
                fx, fy, fz = (
                    table[pl.ds(start + g * 24 + c, 8, stride=3), :] for c in range(3)
                )
                dx = fx - here[0][g]
                dy = fy - here[1][g]
                reach = 1.0 / lax.rsqrt(dx * dx + dy * dy) + reach_offset
                best[g] = jnp.maximum(best[g], (fz - here[2][g]) / reach)
        line = pl.ds(a, 1)
        cx, cy, cz, tans = (sun_ref[c, line, :] for c in range(4))
        for g in range(n // 8):
            at = slice(g * 8, g * 8 + 8)
            incidence = cx * facts[3, at, :] + cy * facts[4, at, :] + cz * facts[5, at, :]
            shade = jax.nn.sigmoid((tans - best[g]) / shade_width)
            direct = solar_flux * jnp.maximum(incidence, 0.0) * shade
            put = pl.ds(pl.multiple_of(a * n + g * 8, 8), 8)
            direct_ref[put, :] = direct
            lit_ref[put, :] = facts[7, at, :] * direct + emissivity * fourth(facts[8, at, :])

    shared = epochs // 4
    core = me & 1
    partner = me ^ 1

    def azimuth(order):
        return ((me // quarter) ^ (order // quarter)) * quarter + (order & (quarter - 1))

    def swap(ref, which):
        return pltpu.make_async_remote_copy(
            src_ref=ref,
            dst_ref=ref,
            send_sem=sent.at[2 + which],
            recv_sem=got.at[n_recv + 4 + which],
            device_id=device(partner),
            device_id_type=pl.DeviceIdType.MESH,
        )

    def swaps(first, facet):
        start = pl.multiple_of(azimuth(first) * n, 8)
        lines = [direct_ref.at[pl.ds(start + k * n + facet, 1)] for k in range(shared)]
        return [swap(lit_ref.at[pl.ds(start, shared * n)], 0)] + [swap(line, 1) for line in lines]

    swapped = (swap(lit_ref.at[pl.ds(0, shared * n)], 0), swap(direct_ref.at[pl.ds(0, shared)], 1))

    def horizons(i, carry):
        @pl.when(i == shared // PAIR)
        def _():
            for copy in swaps(core * shared, partner):
                copy.start()

        @pl.when(i == 2 * shared // PAIR)
        def _():
            to_scalars(3).wait()

        first = jnp.where(i < shared // PAIR, core * shared, shared) + i * PAIR
        for j in range(PAIR):
            horizon(azimuth(first + j))
        return carry

    lax.fori_loop(0, 3 * shared // PAIR, horizons, 0)
    for copy in swapped:
        copy.wait_recv()

    total = jnp.zeros((epochs, width), jnp.float32)
    for p in range(n):
        total = total + lax.dot_general(
            lit_ref[pl.ds(p, epochs, stride=n), :].astype(jnp.bfloat16),
            view[p],
            (((1,), (1,)), ((), ())),
            preferred_element_type=jnp.float32,
        )
    bounce_ref[...] = total
    keep = surface_gain * (1.0 - facts[7, own, :])
    heat_ref[...] = keep * (direct_ref[pl.ds(me, epochs, stride=n), :] + total)
    remote(pl.ds(0, n - 1), me ^ 1, 0).wait_send()
    samples_of(0, n - 1).wait_send()
    for copy in swapped:
        copy.wait_send()


def conduct(bounce_in, heat_ref, cond_ref, soil_ref, final_ref, bounce_ref):
    layers, width = soil_ref.shape
    epochs = heat_ref.shape[0]
    bounce_ref[...] = bounce_in[...]
    cond = cond_ref[...]
    first = lax.broadcasted_iota(jnp.int32, (layers, width), 0) == 0
    last = lax.broadcasted_iota(jnp.int32, (layers, width), 0) == layers - 1

    def advance(t, temps):
        below = jnp.where(last, temps, pltpu.roll(temps, layers - 1, 0))
        above = jnp.where(first, temps, pltpu.roll(temps, 1, 0))
        temps = temps + cond * ((below - temps) - (temps - above))
        gain = heat_ref[pl.ds(t, 1), :] - (surface_gain * emissivity) * fourth(temps)
        return jnp.where(first, temps + gain, temps)

    temps = soil_ref[...]
    if epochs <= 16:
        for t in range(epochs):
            temps = advance(t, temps)
    else:
        temps = lax.fori_loop(0, epochs, advance, temps)
    final_ref[...] = temps


def body(positions, normals, area, albedo, conductivity, soil, sun_tan, samples, occupancy):
    n_recv = lax.axis_size("recv")
    n_src = lax.axis_size("src")
    n = n_recv * n_src
    width = positions.shape[1]
    epochs = sun_tan.shape[0]
    vmem = pl.BlockSpec(memory_space=pltpu.VMEM)
    f32 = jnp.float32
    n_samples = samples.shape[1]
    if n <= 16:
        program = step
        scratch = [
            pltpu.VMEM((1, epochs), f32),
            pltpu.SMEM((1, occupancy.shape[1]), jnp.int32),
            pltpu.VMEM((9, n, width), f32),
            pltpu.VMEM((n, 1, n_samples), jnp.int32),
            pltpu.SMEM((n, 1, n_samples), jnp.int32),
            pltpu.VMEM((3 * (n + 16), width), f32),
            pltpu.VMEM((3 * width * (2 * n + 8) + 8, width), f32),
            pltpu.VMEM((6, width, width), f32),
            pltpu.VMEM((n, width, width), jnp.bfloat16),
            pltpu.VMEM((4, epochs, width), f32),
            pltpu.VMEM((epochs * n, width), f32),
            pltpu.VMEM((epochs * n, width), f32),
            pltpu.SemaphoreType.REGULAR((n_recv,)),
            pltpu.SemaphoreType.DMA((4,)),
            pltpu.SemaphoreType.DMA((n_recv + 6,)),
            pltpu.SemaphoreType.DMA((8,)),
        ]
    else:
        program = kernel
        scratch = [
            pltpu.VMEM((3, width), f32),
            pltpu.VMEM((3, width), f32),
            pltpu.VMEM((1, width), f32),
            pltpu.VMEM((1, width), f32),
            pltpu.VMEM((1, epochs), f32),
            pltpu.VMEM((1, n_samples), jnp.int32),
            pltpu.SMEM((1, occupancy.shape[1]), jnp.int32),
            pltpu.VMEM((n, 4, width), f32),
            pltpu.VMEM((n, 4, width), f32),
            pltpu.VMEM((3, n, width), f32),
            pltpu.VMEM((2 * n, width), f32),
            pltpu.VMEM((6, width, width), f32),
            pltpu.VMEM((n, width, width), jnp.bfloat16),
            pltpu.VMEM((epochs, width), f32),
            pltpu.VMEM((epochs, width), f32),
            pltpu.VMEM((epochs, width), f32),
            pltpu.VMEM((n, epochs // GROUP, GROUP, width), jnp.bfloat16),
            pltpu.SemaphoreType.DMA((6,)),
            pltpu.SemaphoreType.DMA((9,)),
        ]
    held = pl.pallas_call(
        functools.partial(program, n_recv, n_src),
        out_shape=(
            pltpu.VMEM((epochs, width), f32),
            pltpu.VMEM((epochs, width), f32),
            pltpu.VMEM((1, width), f32),
            pltpu.VMEM(soil.shape, f32),
        ),
        in_specs=[pl.BlockSpec(memory_space=pl.ANY)] * 9,
        out_specs=(vmem,) * 4,
        scratch_shapes=scratch,
        compiler_params=pltpu.CompilerParams(collective_id=0, has_side_effects=True),
    )(
        positions,
        normals,
        area.reshape(1, width),
        albedo.reshape(1, width),
        conductivity.reshape(1, width),
        soil,
        sun_tan.reshape(1, epochs),
        samples,
        occupancy,
    )
    return pl.pallas_call(
        conduct,
        out_shape=(
            jax.ShapeDtypeStruct(soil.shape, f32),
            jax.ShapeDtypeStruct((epochs, width), f32),
        ),
        in_specs=[vmem] * 4,
        out_specs=(vmem, vmem),
    )(*(pltpu.with_memory_space_constraint(value, pltpu.VMEM) for value in held))


def solution(mesh):
    in_specs = (
        P(None, ("basin", "recv", "src")),
        P(None, ("basin", "recv", "src")),
        P(("basin", "recv", "src")),
        P(("basin", "recv", "src")),
        P(("basin", "recv", "src")),
        P(None, ("basin", "recv", "src")),
        P(),
        P(("basin", "recv", "src"), None),
        P("basin", None),
    )
    out_specs = (P(None, ("basin", "recv", "src")), P(None, ("basin", "recv", "src")))
    return jax.shard_map(body, mesh=mesh, in_specs=in_specs, out_specs=out_specs, check_vma=False)
```
